32 devices in a mesh: fsdp: 32 (over z, y, x, core).
Axes of the slice: x: 2, y: 2, z: 4, core: 2. Of those that a mesh axis runs over, the one named last changes fastest.
Arguments:
- inputs: bfloat16 [256, 197, 384], P('fsdp'), may hold values from -6 to 6
- out_grad: bfloat16 [256, 197, 384], P('fsdp'), may hold values from -6 to 6
- live_counts: int32 [128], P('fsdp'), may hold values from 1 to 2, 192 in all
- norm1_gain: bfloat16 [2, 384], P(None, 'fsdp'), may hold values from 0.5 to 1.5
- norm1_bias: bfloat16 [2, 384], P(None, 'fsdp'), may hold values from -3 to 3
- w_qkv: bfloat16 [2, 384, 1152], P(None, 'fsdp'), may hold values from -0.3125 to 0.3125
- bias_qv: bfloat16 [2, 768], P(None, 'fsdp'), may hold values from -3 to 3
- w_proj: bfloat16 [2, 384, 384], P(None, 'fsdp'), may hold values from -1.25 to 1.25
- bias_proj: bfloat16 [2, 384], P(None, 'fsdp'), may hold values from -3 to 3
- norm2_gain: bfloat16 [2, 384], P(None, 'fsdp'), may hold values from 0.5 to 1.5
- norm2_bias: bfloat16 [2, 384], P(None, 'fsdp'), may hold values from -3 to 3
- w_fc1: bfloat16 [2, 384, 1536], P(None, 'fsdp'), may hold values from -0.3125 to 0.3125
- bias_fc1: bfloat16 [2, 1536], P(None, 'fsdp'), may hold values from -3 to 3
- w_fc2: bfloat16 [2, 1536, 384], P(None, 'fsdp'), may hold values from -0.15625 to 0.15625
- bias_fc2: bfloat16 [2, 384], P(None, 'fsdp'), may hold values from -3 to 3
Outputs:
- outputs: bfloat16 [256, 197, 384], P('fsdp')
- in_grad: float32 [256, 197, 384], P('fsdp')
- grad_norm1_gain: float32 [2, 384], P(None, 'fsdp')
- grad_norm1_bias: float32 [2, 384], P(None, 'fsdp')
- grad_w_qkv: float32 [2, 384, 1152], P(None, 'fsdp')
- grad_bias_qv: float32 [2, 768], P(None, 'fsdp')
- grad_w_proj: float32 [2, 384, 384], P(None, 'fsdp')
- grad_bias_proj: float32 [2, 384], P(None, 'fsdp')
- grad_norm2_gain: float32 [2, 384], P(None, 'fsdp')
- grad_norm2_bias: float32 [2, 384], P(None, 'fsdp')
- grad_w_fc1: float32 [2, 384, 1536], P(None, 'fsdp')
- grad_bias_fc1: float32 [2, 1536], P(None, 'fsdp')
- grad_w_fc2: float32 [2, 1536, 384], P(None, 'fsdp')
- grad_bias_fc2: float32 [2, 384], P(None, 'fsdp')
The draws below stay inside these ranges and needn't reach their ends.
Inputs may be any that keep to these rules, and one draw needn't show every extreme that they name: `live_counts`: slots at or beyond the count of a micro-batch hold padding.
All inputs are finite; a program needn't handle non-finite values. No bound on the sum of `live_counts` on one device may be relied on, other than what follows from the above.
Results may differ from the reference program's by a relative error of at most 0.012.
Values may be sent and summed in bfloat16 or wider, within the bound.
A program may use at most 256 MiB of HBM per device.

```python
import math
import jax
import jax.numpy as jnp
import numpy as np
from jax import lax

HEAD_DIM = 64
D = 384
FF = 1536
SEQ = 197
LAYERS = 2
MB = 4
SLOTS = 2
SLOTS_ALL = 256
LIVE_TOTAL = 192
N_FSDP = 32


def block_scale(key, extent, split, smallest, largest):
    loudness, own = 1.0, jax.random.fold_in(key, 6)
    for position, parts in split:
        heights = jnp.exp(jax.random.uniform(jax.random.fold_in(own, position), (parts,), jnp.float32, smallest / len(split), largest / len(split)))
        loudness = loudness * jnp.repeat(heights, extent[position] // parts).reshape([-1 if axis == position else 1 for axis in range(len(extent))])
    return loudness


def profile(amount, total, bound, skew):
    portions = [(1 << 20) // math.isqrt(rank ** skew) + 1 for rank in range(2, amount + 1)]
    rest, counts = total - bound - (amount - 1), [1] * (amount - 1)
    while rest > 0:
        movable = [i for i in range(amount - 1) if counts[i] < bound]
        whole, budget = sum([portions[i] for i in movable]), rest
        for i in movable:
            addition = min(bound - counts[i], max(1, budget * portions[i] // whole), rest)
            counts[i] = counts[i] + addition
            rest = rest - addition
    return np.array([bound] + counts)


def ragged_sizes(key, number_of, total, bound, skew):
    if number_of == 2:
        one = jax.random.randint(key, (), max(1, total - bound), min(bound, total - 1) + 1)
        return jnp.stack([one, total - one])
    tallies = jnp.asarray(profile(number_of, total, bound, skew), jnp.int32)
    couples = (number_of - 1) // 2
    source_of, sink = tallies[1:1 + 2 * couples:2], tallies[2:2 + 2 * couples:2]
    margin = jnp.minimum(source_of - 1, bound - sink)
    moved = jax.random.randint(jax.random.fold_in(key, 1), (couples,), 0, 1 << 20) % (margin + 1)
    tallies = tallies.at[1:1 + 2 * couples:2].set(source_of - moved).at[2:2 + 2 * couples:2].set(sink + moved)
    return tallies[jax.random.permutation(jax.random.fold_in(key, 2), number_of)]


def centred(key, dims, spread, most, cuts=(), kind=jnp.bfloat16):
    entries = spread * jax.random.normal(key, dims, jnp.float32)
    if cuts:
        entries = entries * block_scale(key, dims, cuts, -0.22, 0.18)
    return jnp.clip(entries, -most, most).astype(kind)


def setup_inputs(seed: int = 0) -> dict:
    key_list = jax.random.split(jax.random.key(seed), 16)
    return {
        "inputs": centred(key_list[0], (SLOTS_ALL, SEQ, D), 1.0, 6.0, ((0, 32),)),
        "out_grad": centred(key_list[1], (SLOTS_ALL, SEQ, D), 1.0, 6.0, ((0, 32),)),
        "live_counts": ragged_sizes(key_list[2], N_FSDP * MB, LIVE_TOTAL, SLOTS, 1).astype(jnp.int32),
        "norm1_gain": jnp.clip(1.0 + 0.1 * jax.random.normal(key_list[3], (LAYERS, D), jnp.float32), 0.5, 1.5).astype(jnp.bfloat16),
        "norm1_bias": centred(key_list[4], (LAYERS, D), 0.5, 3.0, ((1, 32),)),
        "w_qkv": centred(key_list[5], (LAYERS, D, 3 * D), D ** -0.5, 0.3125, ((1, 32),)),
        "bias_qv": centred(key_list[6], (LAYERS, 2 * D), 0.5, 3.0, ((1, 32),)),
        "w_proj": centred(key_list[7], (LAYERS, D, D), (D // 16) ** -0.5, 1.25, ((1, 32),)),
        "bias_proj": centred(key_list[8], (LAYERS, D), 0.5, 3.0, ((1, 32),)),
        "norm2_gain": jnp.clip(1.0 + 0.1 * jax.random.normal(key_list[9], (LAYERS, D), jnp.float32), 0.5, 1.5).astype(jnp.bfloat16),
        "norm2_bias": centred(key_list[10], (LAYERS, D), 0.5, 3.0, ((1, 32),)),
        "w_fc1": centred(key_list[11], (LAYERS, D, FF), D ** -0.5, 0.3125, ((1, 32),)),
        "bias_fc1": centred(key_list[12], (LAYERS, FF), 0.5, 3.0, ((1, 32),)),
        "w_fc2": centred(key_list[13], (LAYERS, FF, D), FF ** -0.5, 0.15625, ((1, 32),)),
        "bias_fc2": centred(key_list[14], (LAYERS, D), 0.5, 3.0, ((1, 32),)),
    }


EPS = 1e-06

def matmul(left, weight):
    in_shape = left.shape
    result = jnp.dot(left.reshape(-1, in_shape[-1]), weight, preferred_element_type=jnp.float32)
    return result.reshape(in_shape[:-1] + (weight.shape[-1],))

def weight_grad(left, right):
    return jnp.dot(left.reshape(-1, left.shape[-1]).T, right.reshape(-1, right.shape[-1]), preferred_element_type=jnp.float32)

def mix_heads(form, left, right):
    return jnp.einsum(form, left.astype(jnp.float32), right.astype(jnp.float32))

def norm_forward(hidden, gain_row, shift_row):
    mean_row = lax.optimization_barrier(jnp.mean(hidden, axis=-1, keepdims=True))
    centered = hidden - mean_row
    inv_std = lax.rsqrt(lax.optimization_barrier(jnp.mean(centered * centered, axis=-1, keepdims=True)) + EPS)
    normed = centered * inv_std
    return (normed, inv_std, normed * gain_row.astype(jnp.float32) + shift_row.astype(jnp.float32))

def norm_backward(grad_in, normed, inv_std, gain_row):
    gain_grad = lax.optimization_barrier(jnp.sum(grad_in * normed, axis=(0, 1)))
    shift_grad = lax.optimization_barrier(jnp.sum(grad_in, axis=(0, 1)))
    dnorm = grad_in * gain_row.astype(jnp.float32)
    back = inv_std * (dnorm - lax.optimization_barrier(jnp.mean(dnorm, axis=-1, keepdims=True)) - normed * lax.optimization_barrier(jnp.mean(dnorm * normed, axis=-1, keepdims=True)))
    return (back, gain_grad, shift_grad)

def gelu_exact(value):
    return 0.5 * value * (1.0 + lax.erf(value * 0.7071067811865476))

def gelu_slope(value):
    return 0.5 * (1.0 + lax.erf(value * 0.7071067811865476)) + value * jnp.exp(-0.5 * value * value) * 0.3989422804014327

def layer_forward(hidden, params):
    norm1_gain, norm1_bias, w_qkv, bias_qv, w_proj, bias_proj, norm2_gain, norm2_bias, w_fc1, bias_fc1, w_fc2, bias_fc2 = params
    slot_count, length, feat_width = hidden.shape
    head_count = feat_width // HEAD_DIM
    split_shape = (slot_count, length, head_count, HEAD_DIM)
    normed1, inv_std1, shifted1 = norm_forward(hidden, norm1_gain, norm1_bias)
    attn_in = shifted1.astype(jnp.bfloat16)
    project = matmul(attn_in, w_qkv)
    bias_full = bias_qv.astype(jnp.float32)
    query_rows = (project[..., :feat_width] + bias_full[:feat_width]).astype(jnp.bfloat16).reshape(split_shape)
    key_rows = project[..., feat_width:2 * feat_width].astype(jnp.bfloat16).reshape(split_shape)
    value_rows = (project[..., 2 * feat_width:] + bias_full[feat_width:]).astype(jnp.bfloat16).reshape(split_shape)
    scores = mix_heads('bqhd,bkhd->bhqk', query_rows, key_rows) * HEAD_DIM ** (-0.5)
    top_score = lax.optimization_barrier(jnp.max(scores, axis=-1, keepdims=True))
    exp_terms = jnp.exp(scores - top_score)
    exp_total = lax.optimization_barrier(jnp.sum(exp_terms, axis=-1, keepdims=True))
    log_total = top_score + jnp.log(exp_total)
    prob_rows = (exp_terms / exp_total).astype(jnp.bfloat16)
    context = mix_heads('bhqk,bkhd->bqhd', prob_rows, value_rows).astype(jnp.bfloat16).reshape(slot_count, length, feat_width)
    mid_stream = hidden + matmul(context, w_proj) + bias_proj.astype(jnp.float32)
    normed2, inv_std2, shifted2 = norm_forward(mid_stream, norm2_gain, norm2_bias)
    mlp_in = shifted2.astype(jnp.bfloat16)
    pre_act = matmul(mlp_in, w_fc1) + bias_fc1.astype(jnp.float32)
    activated = gelu_exact(pre_act).astype(jnp.bfloat16)
    output = mid_stream + matmul(activated, w_fc2) + bias_fc2.astype(jnp.float32)
    saved_state = (normed1, inv_std1, attn_in, query_rows, key_rows, value_rows, log_total, context, normed2, inv_std2, mlp_in, pre_act, activated)
    return (output, saved_state)

def layer_backward(grad_h, params, saved_state):
    norm1_gain, norm1_bias, w_qkv, bias_qv, w_proj, bias_proj, norm2_gain, norm2_bias, w_fc1, bias_fc1, w_fc2, bias_fc2 = params
    normed1, inv_std1, attn_in, query_rows, key_rows, value_rows, log_total, context, normed2, inv_std2, mlp_in, pre_act, activated = saved_state
    slot_count, length, feat_width = grad_h.shape
    head_count = feat_width // HEAD_DIM
    grad_b = grad_h.astype(jnp.bfloat16)
    grad_fc2w = weight_grad(activated, grad_b)
    grad_fc2b = lax.optimization_barrier(jnp.sum(grad_h, axis=(0, 1)))
    grad_act = matmul(grad_b, w_fc2.T)
    grad_pre_f = grad_act * gelu_slope(pre_act)
    grad_fc1b = lax.optimization_barrier(jnp.sum(grad_pre_f, axis=(0, 1)))
    grad_pre = grad_pre_f.astype(jnp.bfloat16)
    grad_fc1w = weight_grad(mlp_in, grad_pre)
    grad_mlp_in = matmul(grad_pre, w_fc1.T)
    back2, grad_n2gain, grad_n2bias = norm_backward(grad_mlp_in, normed2, inv_std2, norm2_gain)
    grad_mid = grad_h + back2
    grad_mid_b = grad_mid.astype(jnp.bfloat16)
    grad_projw = weight_grad(context, grad_mid_b)
    grad_projb = lax.optimization_barrier(jnp.sum(grad_mid, axis=(0, 1)))
    grad_ctx = matmul(grad_mid_b, w_proj.T).astype(jnp.bfloat16).reshape(slot_count, length, head_count, HEAD_DIM)
    scores = mix_heads('bqhd,bkhd->bhqk', query_rows, key_rows) * HEAD_DIM ** (-0.5)
    probs_f = jnp.exp(scores - log_total)
    probs_b = probs_f.astype(jnp.bfloat16)
    grad_probs = mix_heads('bqhd,bkhd->bhqk', grad_ctx, value_rows)
    grad_value = mix_heads('bhqk,bqhd->bkhd', probs_b, grad_ctx)
    row_dot = lax.optimization_barrier(jnp.sum(probs_f * grad_probs, axis=-1, keepdims=True))
    grad_scores = (probs_f * (grad_probs - row_dot) * HEAD_DIM ** (-0.5)).astype(jnp.bfloat16)
    grad_query = mix_heads('bhqk,bkhd->bqhd', grad_scores, key_rows)
    grad_key = mix_heads('bhqk,bqhd->bkhd', grad_scores, query_rows)
    flat_shape = (slot_count, length, feat_width)
    grad_query = grad_query.reshape(flat_shape)
    grad_key = grad_key.reshape(flat_shape)
    grad_value = grad_value.reshape(flat_shape)
    grad_qvb = jnp.concatenate([lax.optimization_barrier(jnp.sum(grad_query, axis=(0, 1))), lax.optimization_barrier(jnp.sum(grad_value, axis=(0, 1)))])
    grad_project = jnp.concatenate([grad_query, grad_key, grad_value], axis=-1).astype(jnp.bfloat16)
    grad_qkvw = weight_grad(attn_in, grad_project)
    grad_attn_in = matmul(grad_project, w_qkv.T)
    back1, grad_n1gain, grad_n1bias = norm_backward(grad_attn_in, normed1, inv_std1, norm1_gain)
    grad_below = grad_mid + back1
    layer_grads = (grad_n1gain, grad_n1bias, grad_qkvw, grad_qvb, grad_projw, grad_projb, grad_n2gain, grad_n2bias, grad_fc1w, grad_fc1b, grad_fc2w, grad_fc2b)
    return (grad_below, layer_grads)

def micro_batch(image_rows, grad_rows, live_rows, params):
    hidden = image_rows.astype(jnp.float32)
    saves = []
    for layer_idx in range(LAYERS):
        layer_params = tuple((piece_arr[layer_idx] for piece_arr in params))
        hidden, saved_state = layer_forward(hidden, layer_params)
        saves.append(saved_state)
    live_mask = live_rows[:, None, None]
    outputs = (hidden * live_mask).astype(jnp.bfloat16)
    grad_h = grad_rows.astype(jnp.float32) * live_mask
    grad_list = [None] * LAYERS
    for layer_idx in reversed(range(LAYERS)):
        layer_params = tuple((piece_arr[layer_idx] for piece_arr in params))
        grad_h, layer_grads = layer_backward(grad_h, layer_params, saves[layer_idx])
        grad_list[layer_idx] = layer_grads
    stacked = tuple((jnp.stack([grad_list[layer_idx][which] for layer_idx in range(LAYERS)]) for which in range(12)))
    return (outputs, grad_h, stacked)

def reference(inputs, out_grad, live_counts, norm1_gain, norm1_bias, w_qkv, bias_qv, w_proj, bias_proj, norm2_gain, norm2_bias, w_fc1, bias_fc1, w_fc2, bias_fc2):
    params = (norm1_gain, norm1_bias, w_qkv, bias_qv, w_proj, bias_proj, norm2_gain, norm2_bias, w_fc1, bias_fc1, w_fc2, bias_fc2)
    group_count = live_counts.shape[0]
    slot_count = inputs.shape[0] // group_count
    image_groups = inputs.reshape((group_count, slot_count) + inputs.shape[1:])
    grad_groups = out_grad.reshape((group_count, slot_count) + out_grad.shape[1:])
    live_table = (jnp.arange(slot_count, dtype=jnp.int32)[None, :] < live_counts[:, None]).astype(jnp.float32)
    start = tuple((jnp.zeros(piece_arr.shape, jnp.float32) for piece_arr in params))

    def scan_step(running, group_item):
        image_rows, grad_rows, live_rows = group_item
        outputs, grad_in, stacked = micro_batch(image_rows, grad_rows, live_rows, params)
        return (tuple((total + part for total, part in zip(running, stacked))), (outputs, grad_in))
    running, (out_all, grad_all) = lax.scan(scan_step, start, (image_groups, grad_groups, live_table))
    return (out_all.reshape(inputs.shape), grad_all.reshape(inputs.shape), running[0], running[1], running[2], running[3], running[4], running[5], running[6], running[7], running[8], running[9], running[10], running[11])
```

```python
import functools
import math

import jax
import jax.numpy as jnp
from jax import lax
from jax.experimental import pallas as pl
from jax.experimental.pallas import tpu as pltpu
from jax.sharding import PartitionSpec as P

HEAD_DIM = 64
LAYERS = 2
EPS = 1e-06
BF = jnp.bfloat16
F32 = jnp.float32
NN = (((1,), (0,)), ((), ()))
NT = (((1,), (1,)), ((), ()))
TN = (((0,), (0,)), ((), ()))
KEYS = 256
LANES = 128
VMEM_LIMIT = 63 << 20


N1G, N1B, BPJ, N2G, N2B, BF2, BQV, BF1 = range(8)


MESH_ID = pl.DeviceIdType.MESH
VECS = 8


def torus_shape(devices):
    return {16: (4, 2, 2), 64: (4, 4, 4)}.get(devices // 2, (1, 1, devices // 2))


class Cube:
    def __init__(self, devices):
        self.devices = devices
        self.axes = []
        stride = devices
        self.slots_of = []
        for extent in torus_shape(devices):
            stride //= extent
            if extent > 1:
                self.axes.append((extent, stride))
        self.bits = sum(extent.bit_length() - 1 for extent, _ in self.axes)

    def natural_slot(self, device):
        slot = []
        for extent, stride in self.axes:
            pos = (device // stride) % extent
            slot += [pos // 2, (pos + pos // 2) % 2] if extent == 4 else [pos]
        return tuple(slot) + (device % 2,)

    def position(self):
        me = lax.axis_index("fsdp")
        mine, partners = [], []
        for extent, stride in self.axes:
            pos = (me // stride) % extent
            if extent == 4:
                mine += [pos // 2, (pos + pos // 2) % 2]
                partners += [me + (3 - 2 * pos) * stride, me + (1 - 2 * (pos % 2)) * stride]
            else:
                mine += [pos]
                partners += [me + (1 - 2 * pos) * stride]
        core = me % 2
        return mine + [core], partners + [me + 1 - 2 * core]


def greet(partners):
    barrier = pltpu.get_barrier_semaphore()
    for partner in partners:
        pl.semaphore_signal(barrier, inc=1, device_id=(partner,), device_id_type=MESH_ID)
    pl.semaphore_wait(barrier, len(partners))


def color_pieces(shapes, colors):
    units = [(a, c, -(-rows // 16)) for a, (rows, lanes) in enumerate(shapes) for c in range(lanes // LANES)]
    total = sum(u[2] for u in units)
    pieces = [[] for _ in range(colors)]
    seen = 0
    for a, c, weight in units:
        color = min(colors - 1, (2 * seen + weight) * colors // (2 * total))
        seen += weight
        if pieces[color] and pieces[color][-1][0] == a:
            pieces[color][-1][2] = (c + 1) * LANES
        else:
            pieces[color].append([a, c * LANES, (c + 1) * LANES])
    return pieces


class Gather:
    def __init__(self, cube, mine, partners, sources, slots, send, recv, base):
        self.cube, self.mine, self.partners = cube, mine, partners
        self.sources, self.slots = sources, slots
        self.send, self.recv, self.base = send, recv, base
        self.pieces = color_pieces([s.shape[-2:] for s in slots], cube.bits)
        self.copies = {}
        self.own = tuple(mine)

    @staticmethod
    def semaphores(cube, blocks):
        return sum(map(len, color_pieces(blocks, cube.bits))) * (2 * cube.bits + 1)

    def order(self, color, step):
        return (color + step) % self.cube.bits

    def index(self, free, flipped=None):
        return tuple(
            slice(None) if b in free else (1 - m if b == flipped else m) for b, m in enumerate(self.mine)
        )

    def _start(self, key, color, partner, src_of, dst_index):
        made = []
        for a, lo, hi in self.pieces[color]:
            sem = self.base
            self.base += 1
            copy = pltpu.make_async_remote_copy(
                src_ref=src_of(a, lo, hi),
                dst_ref=self.slots[a].at[dst_index + (slice(None), slice(lo, hi))],
                send_sem=self.send.at[sem],
                recv_sem=self.recv.at[sem],
                device_id=(partner,),
                device_id_type=MESH_ID,
            )
            copy.start()
            made.append(copy)
        self.copies[key, color] = made

    def _wait_recv(self, key, color):
        for copy in self.copies[key, color]:
            copy.wait_recv()

    def step(self, t):
        bits = self.cube.bits
        from_source = lambda a, lo, hi: self.sources[a].at[:, lo:hi]
        for color in range(bits):
            free = {self.order(color, s) for s in range(t)}
            if t > 0:
                self._wait_recv(t - 1, color)
            if t < bits:
                idx = self.index(free)
                from_slots = lambda a, lo, hi: self.slots[a].at[idx + (slice(None), slice(lo, hi))]
                self._start(t, color, self.partners[self.order(color, t)], from_source if t == 0 else from_slots, idx)
        for color in range(bits):
            if t == 0:
                self._start(bits, color, self.partners[-1], from_source, self.own)
            else:
                new = self.order(color, t - 1)
                idx = self.index({self.order(color, s) for s in range(t - 1)}, flipped=new)
                from_slots = lambda a, lo, hi: self.slots[a].at[idx + (slice(None), slice(lo, hi))]
                self._start(bits + t, color, self.partners[-1], from_slots, idx)

    def finish(self):
        bits = self.cube.bits
        for t in range(bits + 1):
            for color in range(bits):
                self._wait_recv(bits + t, color)
        for made in self.copies.values():
            for copy in made:
                copy.wait_send()


class Scatter:
    def __init__(self, cube, mine, partners, slots, inbox, send, recv, base):
        self.cube, self.mine, self.partners = cube, mine, partners
        self.slots, self.inbox = slots, inbox
        self.send, self.recv, self.base = send, recv, base
        self.pieces = color_pieces([s.shape[-2:] for s in slots], cube.bits)
        self.copies = {}

    @staticmethod
    def semaphores(cube, blocks):
        return sum(map(len, color_pieces(blocks, cube.bits))) * (cube.bits + 1)

    def order(self, color, step):
        return (color + step) % self.cube.bits

    def index(self, free, flipped=None):
        return tuple(
            slice(None) if b in free else (1 - m if b == flipped else m) for b, m in enumerate(self.mine)
        )

    def free_of(self, color, t):
        bits = self.cube.bits
        if t == bits:
            return set(range(bits)), bits
        return {self.order(color, s) for s in range(t)}, self.order(color, t)

    def start(self, color, t):
        bits = self.cube.bits
        free, bit = self.free_of(color, t)
        idx = self.index(free, flipped=bit)
        made = []
        for a, lo, hi in self.pieces[color]:
            sem = self.base
            self.base += 1
            copy = pltpu.make_async_remote_copy(
                src_ref=self.slots[a].at[idx + (slice(None), slice(lo, hi))],
                dst_ref=self.inbox[a].at[(t,) + idx[:-1] + (slice(None), slice(lo, hi))],
                send_sem=self.send.at[sem],
                recv_sem=self.recv.at[sem],
                device_id=(self.partners[bit],),
                device_id_type=MESH_ID,
            )
            copy.start()
            made.append(copy)
        self.copies[color, t] = made

    def absorb(self, color, t, outs=None):
        free, bit = self.free_of(color, t)
        for copy in self.copies[color, t]:
            copy.wait_recv()
        for a, lo, hi in self.pieces[color]:
            span = (slice(None), slice(lo, hi))
            for combo in range(1 << len(free)):
                order = sorted(free)
                pick = {b: (combo >> i) & 1 for i, b in enumerate(order)}
                idx = tuple(pick.get(b, m) for b, m in enumerate(self.mine))
                here = self.slots[a][idx + span]
                came = self.inbox[a][(t,) + idx[:-1] + span]
                if t == 0:
                    outs[a][:, lo:hi] = here.astype(F32) + came.astype(F32)
                else:
                    self.slots[a][idx + span] = here + came

    def finish(self):
        for made in self.copies.values():
            for copy in made:
                copy.wait_send()


def spread_blocks(cube, slots, target):
    rows = slots.shape[-2]
    group = 16 // math.gcd(rows, 16)
    for first in range(0, cube.devices, group):
        parts = [slots[cube.natural_slot(d)] for d in range(first, first + group)]
        if rows % 4:
            parts = [p.astype(F32) for p in parts]
        joined = parts[0] if group == 1 else jnp.concatenate(parts, axis=0)
        target[first * rows : (first + group) * rows, :] = joined.astype(target.dtype)


def split_blocks(cube, source, slots):
    rows = slots.shape[-2]
    group = 16 // math.gcd(rows, 16)
    for first in range(0, cube.devices, group):
        block = source[first * rows : (first + group) * rows, :]
        if rows % 4:
            block = block.astype(F32)
        for i in range(group):
            slots[cube.natural_slot(first + i)] = block[i * rows : (i + 1) * rows, :].astype(slots.dtype)


def mm(left, right, dims):
    return lax.dot_general(left, right, dims, preferred_element_type=F32)


def norm_stats(hidden):
    centered = hidden - jnp.mean(hidden, axis=-1, keepdims=True)
    inv_std = lax.rsqrt(jnp.mean(centered * centered, axis=-1, keepdims=True) + EPS)
    return centered * inv_std, inv_std


def norm_back(grad_in, normed, inv_std, gain):
    dnorm = grad_in * gain
    return inv_std * (
        dnorm
        - jnp.mean(dnorm, axis=-1, keepdims=True)
        - normed * jnp.mean(dnorm * normed, axis=-1, keepdims=True)
    )


def half_masks():
    lane = lax.broadcasted_iota(jnp.int32, (1, LANES), 1)
    low = (lane < HEAD_DIM).astype(F32).astype(BF)
    return low, 1 - low


def alive(counts, step, per_step, slots, g):
    count = counts[step * (per_step // slots) + g // slots]
    return jnp.where(g % slots < count, 1.0, 0.0).astype(F32)


def fwd_body(first, last, per_step, slots, seq, rows, live_ref, x_ref, vec_ref, wqkv_ref, wproj_ref, w1_ref, w2_ref, *rest):
    if last:
        (out_ref, n1_ref, inv_ref, qkv_out, e_ref, il_ref, ctx_ref, n2_ref, act_ref, slope_ref, hid, qkv_ref) = rest
    else:
        (out_ref, n1_ref, inv_ref, qkv_out, e_ref, il_ref, ctx_ref, n2_ref, act_ref, slope_ref, hid, qkv_ref) = rest
    step = pl.program_id(0)
    width = wproj_ref.shape[0]
    hidden_ff = w1_ref.shape[1]
    total = per_step * rows

    @pl.when(step == 0)
    def _():
        qkv_ref[total:, :] = jnp.zeros_like(qkv_ref[total:, :])
        if first:
            hid[...] = jnp.zeros_like(hid)

    if first:
        for g in range(per_step):
            hid[g * rows : g * rows + seq, :] = x_ref[g].astype(F32)
        h = hid[...]
    else:
        h = x_ref[...]
    n1, inv1 = norm_stats(h)
    n1_ref[...] = n1.astype(BF)
    attn_in = (n1 * vec_ref[N1G:N1G+1, :width] + vec_ref[N1B:N1B+1, :width]).astype(BF)
    q = mm(attn_in, wqkv_ref[:, :width], NN) + vec_ref[BQV:BQV+1, :width]
    q = q.astype(BF) * BF(HEAD_DIM ** -0.5)
    k = mm(attn_in, wqkv_ref[:, width : 2 * width], NN).astype(BF)
    v = (mm(attn_in, wqkv_ref[:, 2 * width :], NN) + vec_ref[BQV:BQV+1, width : 2 * width]).astype(BF)
    for i, part in enumerate((q, k, v)):
        qkv_ref[0:total, i * width : (i + 1) * width] = part
        qkv_out[:, i * width : (i + 1) * width] = part
    low, high = half_masks()
    lane = lax.broadcasted_iota(jnp.int32, (1, KEYS), 1)
    key_mask = jnp.where(lane < seq, 0.0, -1e30).astype(F32)
    lane_low = lax.broadcasted_iota(jnp.int32, (1, LANES), 1) < HEAD_DIM
    ones = jnp.ones((KEYS, LANES), BF)
    for g in range(per_step):
        r0 = g * rows
        for pair in range(width // LANES):
            c0 = pair * LANES
            qp = qkv_ref[r0 : r0 + rows, c0 : c0 + LANES]
            kp = qkv_ref[r0 : r0 + KEYS, width + c0 : width + c0 + LANES]
            vp = qkv_ref[r0 : r0 + KEYS, 2 * width + c0 : 2 * width + c0 + LANES]
            vo = jnp.concatenate([vp, ones], axis=1)
            parts = []
            for half, mask in enumerate((low, high)):
                s = mm(qp * mask, kp, NT) + key_mask
                e = jnp.exp(s - jnp.max(s, axis=-1, keepdims=True)).astype(BF)
                j = 2 * pair + half
                e_ref[r0 : r0 + rows, j * KEYS : (j + 1) * KEYS] = e
                r = mm(e, vo, NN)
                recip = 1.0 / r[:, LANES:]
                parts.append((r[:, :LANES] * recip, recip))
            ctx_ref[r0 : r0 + rows, c0 : c0 + LANES] = jnp.where(lane_low, parts[0][0], parts[1][0]).astype(BF)
            il_ref[r0 : r0 + rows, c0 : c0 + LANES] = jnp.where(lane_low, parts[0][1], parts[1][1])
    mid = h + mm(ctx_ref[...], wproj_ref[...], NN) + vec_ref[BPJ:BPJ+1, :width]
    n2, inv2 = norm_stats(mid)
    n2_ref[...] = n2.astype(BF)
    inv_ref[...] = jnp.where(lane_low, inv1, inv2)
    mlp_in = (n2 * vec_ref[N2G:N2G+1, :width] + vec_ref[N2B:N2B+1, :width]).astype(BF)
    chunk = 256
    for c in range(0, hidden_ff, chunk):
        pre = mm(mlp_in, w1_ref[:, c : c + chunk], NN) + vec_ref[BF1:BF1+1, c : c + chunk]
        cdf = 0.5 + 0.5 * lax.erf(pre * 0.7071067811865476)
        act_ref[:, c : c + chunk] = (pre * cdf).astype(BF)
        slope_ref[:, c : c + chunk] = (cdf + pre * jnp.exp(-0.5 * pre * pre) * 0.3989422804014327).astype(BF)
    out = mid + mm(act_ref[...], w2_ref[...], NN) + vec_ref[BF2:BF2+1, :width]
    if last:
        hid[...] = out
        for g in range(per_step):
            live = alive(live_ref, step, per_step, slots, g)
            out_ref[g] = (hid[g * rows : g * rows + seq, :] * live).astype(BF)
    else:
        out_ref[...] = out


def bwd_mlp_body(first, per_step, slots, seq, rows, live_ref, gh_ref, vec_ref, w1_ref, w2_ref, n2_ref, inv_ref, slope_ref, act_ref,
                 gm_ref, dw1_ref, dw2_ref, vecs_ref, hid, gb_all, dpre_all, mlp_all, act_all):
    step = pl.program_id(0)
    width = w1_ref.shape[0]
    hidden_ff = w1_ref.shape[1]
    total = per_step * rows
    span = pl.ds(pl.multiple_of(step * total, 16), total)

    @pl.when(step == 0)
    def _():
        vecs_ref[...] = jnp.zeros_like(vecs_ref)
        if first:
            hid[...] = jnp.zeros_like(hid)

    if first:
        for g in range(per_step):
            live = alive(live_ref, step, per_step, slots, g)
            hid[g * rows : g * rows + seq, :] = gh_ref[g].astype(F32) * live
        gh = hid[...]
    else:
        gh = gh_ref[...]
    gb = gh.astype(BF)
    gb_all[span, :] = gb
    act_all[span, :] = act_ref[...]
    vecs_ref[BF2:BF2+1, :width] += jnp.sum(gh, axis=0, keepdims=True)
    chunk = 256
    dmlp = jnp.zeros((total, width), F32)
    for c in range(0, hidden_ff, chunk):
        dpre = mm(gb, w2_ref[c : c + chunk, :], NT) * slope_ref[:, c : c + chunk].astype(F32)
        vecs_ref[BF1:BF1+1, c : c + chunk] += jnp.sum(dpre, axis=0, keepdims=True)
        dpre_all[span, c : c + chunk] = dpre.astype(BF)
    dmlp = mm(dpre_all[span, :], w1_ref[...], NT)
    n2 = n2_ref[...].astype(F32)
    mlp_all[span, :] = (n2 * vec_ref[N2G:N2G+1, :width] + vec_ref[N2B:N2B+1, :width]).astype(BF)
    vecs_ref[N2G:N2G+1, :width] += jnp.sum(dmlp * n2, axis=0, keepdims=True)
    vecs_ref[N2B:N2B+1, :width] += jnp.sum(dmlp, axis=0, keepdims=True)
    gm = gh + norm_back(dmlp, n2, inv_ref[:, HEAD_DIM : HEAD_DIM + 1], vec_ref[N2G:N2G+1, :width])
    gm_ref[...] = gm
    vecs_ref[BPJ:BPJ+1, :width] += jnp.sum(gm, axis=0, keepdims=True)

    @pl.when(step == pl.num_programs(0) - 1)
    def _():
        for c in range(0, hidden_ff, 512):
            dw1_ref[:, c : c + 512] = mm(mlp_all[...], dpre_all[:, c : c + 512], TN).astype(dw1_ref.dtype)
            dw2_ref[c : c + 512, :] = mm(act_all[:, c : c + 512], gb_all[...], TN).astype(dw2_ref.dtype)


def bwd_attn_body(last, per_step, seq, rows, gm_ref, vec_ref, wqkv_ref, wproj_ref, n1_ref, inv_ref, qkv_in, e_ref, il_ref, ctx_ref,
                  gh_ref, dwqkv_ref, dwproj_ref, vecs_ref, hid, qkv_ref, gmb_all, ctx_all, ai_all, dqkv_all):
    step = pl.program_id(0)
    width = wproj_ref.shape[0]
    total = per_step * rows
    base = pl.multiple_of(step * total, 16)
    span = pl.ds(base, total)

    @pl.when(step == 0)
    def _():
        vecs_ref[...] = jnp.zeros_like(vecs_ref)
        qkv_ref[total:, :] = jnp.zeros_like(qkv_ref[total:, :])

    qkv_ref[0:total, :] = qkv_in[...]
    gm = gm_ref[...]
    gmb = gm.astype(BF)
    gmb_all[span, :] = gmb
    ctx_all[span, :] = ctx_ref[...]
    dctx = mm(gmb, wproj_ref[...], NT).astype(BF).astype(F32) * il_ref[...]
    dos_all = dctx.astype(BF)
    doo_all = (dctx * ctx_ref[...].astype(F32)).astype(BF)
    low, high = half_masks()
    minus = jnp.full((KEYS, LANES), -1.0, BF)
    for g in range(per_step):
        r0 = g * rows
        rr = pl.ds(pl.multiple_of(base + r0, 16), rows)
        for pair in range(width // LANES):
            c0 = pair * LANES
            qp = qkv_ref[r0 : r0 + rows, c0 : c0 + LANES]
            kp = qkv_ref[r0 : r0 + KEYS, width + c0 : width + c0 + LANES]
            vp = qkv_ref[r0 : r0 + KEYS, 2 * width + c0 : 2 * width + c0 + LANES]
            vm = jnp.concatenate([vp, minus], axis=1)
            dos = dos_all[r0 : r0 + rows, c0 : c0 + LANES]
            doo = doo_all[r0 : r0 + rows, c0 : c0 + LANES]
            dq = dk = dv = None
            for half, mask in enumerate((low, high)):
                j = 2 * pair + half
                e = e_ref[r0 : r0 + rows, j * KEYS : (j + 1) * KEYS]
                dd = mm(jnp.concatenate([dos * mask, doo * mask], axis=1), vm, NT)
                ds = (e.astype(F32) * dd).astype(BF)
                dv_h = mm(e, dos * mask, TN)
                dk_h = mm(ds, qp * mask, TN)
                dq_h = mm(ds, kp * mask, NN)
                dq = dq_h if dq is None else dq + dq_h
                dk = dk_h if dk is None else dk + dk_h
                dv = dv_h if dv is None else dv + dv_h
            dq = dq * (HEAD_DIM ** -0.5)
            dv = dv[:rows]
            vecs_ref[BQV:BQV+1, c0 : c0 + LANES] += jnp.sum(dq, axis=0, keepdims=True)
            vecs_ref[BQV:BQV+1, width + c0 : width + c0 + LANES] += jnp.sum(dv, axis=0, keepdims=True)
            dqkv_all[rr, c0 : c0 + LANES] = dq.astype(BF)
            dqkv_all[rr, width + c0 : width + c0 + LANES] = dk[:rows].astype(BF)
            dqkv_all[rr, 2 * width + c0 : 2 * width + c0 + LANES] = dv.astype(BF)
    dai = mm(dqkv_all[span, :], wqkv_ref[...], NT)
    n1 = n1_ref[...].astype(F32)
    ai_all[span, :] = (n1 * vec_ref[N1G:N1G+1, :width] + vec_ref[N1B:N1B+1, :width]).astype(BF)
    vecs_ref[N1G:N1G+1, :width] += jnp.sum(dai * n1, axis=0, keepdims=True)
    vecs_ref[N1B:N1B+1, :width] += jnp.sum(dai, axis=0, keepdims=True)
    gh = gm + norm_back(dai, n1, inv_ref[:, 0:1], vec_ref[N1G:N1G+1, :width])
    if last:
        hid[...] = gh
        for g in range(per_step):
            gh_ref[g] = hid[g * rows : g * rows + seq, :]
    else:
        gh_ref[...] = gh

    @pl.when(step == pl.num_programs(0) - 1)
    def _():
        dwproj_ref[...] = mm(ctx_all[...], gmb_all[...], TN).astype(dwproj_ref.dtype)
        for c in range(0, 3 * width, width):
            dwqkv_ref[:, c : c + width] = mm(ai_all[...], dqkv_all[:, c : c + width], TN).astype(dwqkv_ref.dtype)


def full(shape):
    return pl.BlockSpec(shape, lambda i: (0,) * len(shape))


SM = pl.BlockSpec(memory_space=pltpu.SMEM)


def run_layers(x, og, live, params, per_step=2, gdt=BF):
    images, seq, width = x.shape
    slots = images // live.shape[0]
    ff = params[0][3].shape[1]
    rows = -(-seq // 16) * 16
    steps = images // per_step
    blk = per_step * rows
    tot = images * rows
    sd = jax.ShapeDtypeStruct
    rb = lambda n: pl.BlockSpec((blk, n), lambda i: (i, 0))
    ib = pl.BlockSpec((per_step, seq, width), lambda i: (i, 0, 0))
    heads_w = (width // HEAD_DIM) * KEYS
    cp = pltpu.CompilerParams(vmem_limit_bytes=VMEM_LIMIT)
    h = x
    saved = []
    for l in range(LAYERS):
        vec, wqkv, wproj, w1, w2 = params[l]
        first, last = l == 0, l == LAYERS - 1
        outs = pl.pallas_call(
            functools.partial(fwd_body, first, last, per_step, slots, seq, rows),
            grid=(steps,),
            in_specs=[SM, ib if first else rb(width)] + [full(a.shape) for a in (vec, wqkv, wproj, w1, w2)],
            out_specs=[ib if last else rb(width), rb(width), rb(LANES), rb(3 * width), rb(heads_w), rb(width), rb(width), rb(width), rb(ff), rb(ff)],
            out_shape=[sd((images, seq, width), BF) if last else sd((tot, width), F32), sd((tot, width), BF), sd((tot, LANES), F32), sd((tot, 3 * width), BF),
                       sd((tot, heads_w), BF), sd((tot, width), F32), sd((tot, width), BF), sd((tot, width), BF), sd((tot, ff), BF), sd((tot, ff), BF)],
            scratch_shapes=[pltpu.VMEM((blk, width), F32), pltpu.VMEM((blk + KEYS - rows, 3 * width), BF)],
            compiler_params=cp, name=f"fwd{l}",
        )(live, h, vec, wqkv, wproj, w1, w2)
        h = outs[0]
        saved.append(outs[1:])
    result = h
    gh = og
    grads = [None] * LAYERS
    for l in reversed(range(LAYERS)):
        vec, wqkv, wproj, w1, w2 = params[l]
        n1, inv, qkv, e, il, ctx, n2, act, slope = saved[l]
        first, last = l == LAYERS - 1, l == 0
        gm, dw1, dw2, vecs_m = pl.pallas_call(
            functools.partial(bwd_mlp_body, first, per_step, slots, seq, rows),
            grid=(steps,),
            in_specs=[SM, ib if first else rb(width), full(vec.shape), full(w1.shape), full(w2.shape), rb(width), rb(LANES), rb(ff), rb(ff)],
            out_specs=[rb(width), full(w1.shape), full(w2.shape), full(vec.shape)],
            out_shape=[sd((tot, width), F32), sd(w1.shape, gdt), sd(w2.shape, gdt), sd(vec.shape, F32)],
            scratch_shapes=[pltpu.VMEM((blk, width), F32), pltpu.VMEM((tot, width), BF), pltpu.VMEM((tot, ff), BF), pltpu.VMEM((tot, width), BF), pltpu.VMEM((tot, ff), BF)],
            compiler_params=cp, name=f"bwd_mlp{l}",
        )(live, gh, vec, w1, w2, n2, inv, slope, act)
        gh, dwqkv, dwproj, vecs_a = pl.pallas_call(
            functools.partial(bwd_attn_body, last, per_step, seq, rows),
            grid=(steps,),
            in_specs=[rb(width), full(vec.shape), full(wqkv.shape), full(wproj.shape), rb(width), rb(LANES), rb(3 * width), rb(heads_w), rb(width), rb(width)],
            out_specs=[ib if last else rb(width), full(wqkv.shape), full(wproj.shape), full(vec.shape)],
            out_shape=[sd((images, seq, width), F32) if last else sd((tot, width), F32), sd(wqkv.shape, gdt), sd(wproj.shape, gdt), sd(vec.shape, F32)],
            scratch_shapes=[pltpu.VMEM((blk, width), F32), pltpu.VMEM((blk + KEYS - rows, 3 * width), BF), pltpu.VMEM((tot, width), BF), pltpu.VMEM((tot, width), BF), pltpu.VMEM((tot, width), BF), pltpu.VMEM((tot, 3 * width), BF)],
            compiler_params=cp, name=f"bwd_attn{l}",
        )(gm, vec, wqkv, wproj, n1, inv, qkv, e, il, ctx)
        grads[l] = (vecs_m, vecs_a, dwqkv, dwproj, dw1, dw2)
    return result, gh, grads


def gather_body(cube, refs):
    count = 12
    args, outs, scratch = refs[:count], refs[count : count + 5 * LAYERS], refs[count + 5 * LAYERS :]
    (norm1_gain, norm1_bias, w_qkv, bias_qv, w_proj, bias_proj, norm2_gain, norm2_bias, w_fc1, bias_fc1, w_fc2, bias_fc2) = args
    vectors = (norm1_gain, norm1_bias, bias_proj, norm2_gain, norm2_bias, bias_fc2, bias_qv, bias_fc1)
    pack, send, recv, local = scratch[:4]
    slots = [scratch[4 + 5 * layer : 9 + 5 * layer] for layer in range(LAYERS)]
    pack[...] = jnp.zeros_like(pack)
    for layer in range(LAYERS):
        for i, vector in enumerate(vectors):
            pack[layer, i : i + 1, : vector.shape[1]] = vector[layer : layer + 1, :].astype(F32)
    mine, partners = cube.position()
    greet(partners)
    gathers, copies = [], []
    for layer in range(LAYERS):
        sources = [pack.at[layer]] + [w.at[layer] for w in (w_qkv, w_proj, w_fc1, w_fc2)]
        gathers.append(Gather(cube, mine, partners, sources, slots[layer], send, recv, layer * send.shape[0] // LAYERS))
        for i, source in enumerate(sources):
            copies.append(pltpu.make_async_copy(source, slots[layer][i].at[tuple(mine)], local.at[5 * layer + i]))
    for copy in copies:
        copy.start()
    for tick in range(cube.bits + LAYERS):
        if tick == 1:
            for copy in copies:
                copy.wait()
        for layer in range(LAYERS):
            if 0 <= tick - layer <= cube.bits:
                gathers[layer].step(tick - layer)
    for layer in range(LAYERS):
        gathers[layer].finish()
        vec_out, wqkv_out, wproj_out, w1_out, w2_out = outs[5 * layer : 5 * layer + 5]
        vec_out[...] = jnp.zeros_like(vec_out)
        spread_vectors(cube, slots[layer][0], [v.shape[1] for v in vectors], vec_out)
        for slot, out in zip(slots[layer][1:], (wqkv_out, wproj_out, w1_out, w2_out)):
            spread_blocks(cube, slot, out)


def vector_runs(sizes):
    runs = []
    for i, size in enumerate(sizes):
        if runs and runs[-1][2] == size:
            runs[-1][1] = i + 1
        else:
            runs.append([i, i + 1, size])
    return runs


def spread_vectors(cube, slots, sizes, target):
    for d in range(cube.devices):
        for lo, hi, size in vector_runs(sizes):
            target[lo:hi, d * size : (d + 1) * size] = slots[cube.natural_slot(d) + (slice(lo, hi), slice(0, size))]


def split_vectors(cube, source, sizes, slots):
    for d in range(cube.devices):
        for lo, hi, size in vector_runs(sizes):
            slots[cube.natural_slot(d) + (slice(lo, hi), slice(0, size))] = source[lo:hi, d * size : (d + 1) * size]


def scatter_body(cube, sizes, refs):
    grads, outs, scratch = refs[: 6 * LAYERS], refs[6 * LAYERS : 6 * LAYERS + 12], refs[6 * LAYERS + 12 :]
    (norm1_gain, norm1_bias, w_qkv, bias_qv, w_proj, bias_proj, norm2_gain, norm2_bias, w_fc1, bias_fc1, w_fc2, bias_fc2) = outs
    vectors = (norm1_gain, norm1_bias, bias_proj, norm2_gain, norm2_bias, bias_fc2, bias_qv, bias_fc1)
    send, recv, pack, sums = scratch[:4]
    bufs = [scratch[4 + 10 * layer : 14 + 10 * layer] for layer in range(LAYERS)]
    mine, partners = cube.position()
    greet(partners)
    scatters = []
    for layer in reversed(range(LAYERS)):
        vec_m, vec_a, *weights = grads[6 * layer : 6 * layer + 6]
        slots, inbox = bufs[layer][:5], bufs[layer][5:]
        sums[...] = vec_m[...] + vec_a[...]
        slots[0][...] = jnp.zeros_like(slots[0])
        split_vectors(cube, sums, sizes, slots[0])
        for slot, weight in zip(slots[1:], weights):
            split_blocks(cube, weight, slot)
        work = Scatter(cube, mine, partners, slots, inbox, send, recv, layer * send.shape[0] // LAYERS)
        scatters.append((layer, work))
        for color in range(cube.bits):
            work.start(color, cube.bits)
    for t in reversed(range(cube.bits)):
        for layer, work in scatters:
            for color in range(cube.bits):
                work.absorb(color, t + 1)
                work.start(color, t)
    for layer, work in scatters:
        targets = [pack.at[layer], w_qkv.at[layer], w_proj.at[layer], w_fc1.at[layer], w_fc2.at[layer]]
        for color in range(cube.bits):
            work.absorb(color, 0, targets)
        work.finish()
        for i, vector in enumerate(vectors):
            vector[layer : layer + 1, :] = pack[layer, i : i + 1, : vector.shape[1]]


def slot_shapes(cube, blocks):
    lead = (2,) * (cube.bits + 1)
    return [pltpu.VMEM(lead + b, F32 if i == 0 else BF) for i, b in enumerate(blocks)]


def inbox_shapes(cube, blocks):
    lead = (cube.bits + 1,) + (2,) * cube.bits
    return [pltpu.VMEM(lead + b, F32 if i == 0 else BF) for i, b in enumerate(blocks)]


def per_device(devices, inputs, out_grad, live_counts, *params):
    cube = Cube(devices)
    w_qkv, w_proj, w_fc1, w_fc2 = (params[i] for i in (2, 4, 8, 10))
    sizes = [params[i].shape[1] for i in (0, 1, 5, 6, 7, 11, 3, 9)]
    ff = params[9].shape[1] * devices
    blocks = [(VECS, LANES)] + [w.shape[1:] for w in (w_qkv, w_proj, w_fc1, w_fc2)]
    sd = jax.ShapeDtypeStruct
    any_spec = pl.BlockSpec(memory_space=pl.ANY)
    vmem = pl.BlockSpec(memory_space=pltpu.VMEM)
    wide = lambda b: (b[0] * devices, b[1])
    layer_outs = [sd((VECS, ff), F32)] + [sd(wide(b), BF) for b in blocks[1:]]
    gathered = pl.pallas_call(
        lambda *refs: gather_body(cube, refs),
        in_specs=[any_spec if p.ndim == 3 else vmem for p in params],
        out_specs=[vmem] * (5 * LAYERS),
        out_shape=layer_outs * LAYERS,
        scratch_shapes=[
            pltpu.VMEM((LAYERS, VECS, LANES), F32),
            pltpu.SemaphoreType.DMA((LAYERS * Gather.semaphores(cube, blocks),)),
            pltpu.SemaphoreType.DMA((LAYERS * Gather.semaphores(cube, blocks),)),
            pltpu.SemaphoreType.DMA((5 * LAYERS,)),
        ]
        + slot_shapes(cube, blocks) * LAYERS,
        compiler_params=pltpu.CompilerParams(collective_id=0, has_side_effects=True, vmem_limit_bytes=VMEM_LIMIT),
        name="gather",
    )(*params)
    layers = [gathered[5 * layer : 5 * layer + 5] for layer in range(LAYERS)]
    outputs, in_grad, grads = run_layers(inputs, out_grad, live_counts, layers)
    summed = pl.pallas_call(
        lambda *refs: scatter_body(cube, sizes, refs),
        in_specs=[vmem] * (6 * LAYERS),
        out_specs=[vmem] * 12,
        out_shape=[sd(p.shape, F32) for p in params],
        scratch_shapes=[
            pltpu.SemaphoreType.DMA((LAYERS * Scatter.semaphores(cube, blocks),)),
            pltpu.SemaphoreType.DMA((LAYERS * Scatter.semaphores(cube, blocks),)),
            pltpu.VMEM((LAYERS, VECS, LANES), F32),
            pltpu.VMEM((VECS, ff), F32),
        ]
        + (slot_shapes(cube, blocks) + inbox_shapes(cube, blocks)) * LAYERS,
        compiler_params=pltpu.CompilerParams(collective_id=1, has_side_effects=True, vmem_limit_bytes=VMEM_LIMIT),
        name="scatter",
    )(*[g for layer in grads for g in layer])
    return (outputs, in_grad, *summed)


def solution(mesh):
    devices = mesh.shape["fsdp"]
    rows3, flat2, rows2 = P("fsdp", None, None), P(None, "fsdp"), P(None, "fsdp", None)
    param_specs = (flat2, flat2, rows2, flat2, rows2, flat2, flat2, flat2, rows2, flat2, rows2, flat2)
    return jax.shard_map(
        functools.partial(per_device, devices),
        mesh=mesh,
        in_specs=(rows3, rows3, P("fsdp")) + param_specs,
        out_specs=(rows3, rows3) + param_specs,
        check_vma=False,
    )
```

```python
import functools
import math

import jax
import jax.numpy as jnp
from jax import lax
from jax.experimental import pallas as pl
from jax.experimental.pallas import tpu as pltpu
from jax.sharding import PartitionSpec as P

HEAD_DIM = 64
LAYERS = 2
EPS = 1e-06
BF = jnp.bfloat16
F32 = jnp.float32
NN = (((1,), (0,)), ((), ()))
NT = (((1,), (1,)), ((), ()))
TN = (((0,), (0,)), ((), ()))
KEYS = 256
LANES = 128
VMEM_LIMIT = 67_000_000
PER_STEP = 2
MESH_ID = pl.DeviceIdType.MESH
N1G, N1B, BPJ, BQV, N2G, N2B, BF2, BF1 = range(8)
VECS = 8
ATTN, MLP = 0, 1
COLORS = 2


def torus_shape(devices):
    return {16: (4, 2, 2), 64: (4, 4, 4)}.get(devices // 2, (1, 1, devices // 2))


class Cube:
    def __init__(self, devices):
        self.devices = devices
        self.axes = []
        stride = devices
        for extent in torus_shape(devices):
            stride //= extent
            if extent > 1:
                self.axes.append((extent, stride))
        by_axis, self.bits = [], 0
        for extent, _ in self.axes:
            count = extent.bit_length() - 1
            by_axis.append(list(range(self.bits, self.bits + count)))
            self.bits += count
        self.slots = 1 << self.bits
        orders = [by_axis, by_axis[:1] + by_axis[:0:-1]]
        self.orders = [sum(order, []) for order in orders]

    def bits_of(self, device):
        bits = []
        for extent, stride in self.axes:
            pos = (device // stride) % extent
            bits += [pos // 2, (pos + pos // 2) % 2] if extent == 4 else [pos]
        return bits

    def order(self, color, step):
        return self.orders[color][step]

    def flat(self, color, bits, first=0):
        return sum(bits[self.order(color, s)] * (1 << s) for s in range(first, self.bits))

    def place(self, color, device):
        return device % 2, color, self.flat(color, self.bits_of(device))

    def position(self):
        me = lax.axis_index("fsdp")
        partners = []
        for extent, stride in self.axes:
            pos = (me // stride) % extent
            if extent == 4:
                partners += [me + (3 - 2 * pos) * stride, me + (1 - 2 * (pos % 2)) * stride]
            else:
                partners += [me + (1 - 2 * pos) * stride]
        return self.bits_of(me), me % 2, partners, me + 1 - 2 * (me % 2)


def greet(partners):
    barrier = pltpu.get_barrier_semaphore()
    for partner in partners:
        pl.semaphore_signal(barrier, inc=1, device_id=(partner,), device_id_type=MESH_ID)
    pl.semaphore_wait(barrier, len(partners))


class Group:
    def __init__(self, cube, shapes, sizes):
        self.cube, self.sizes = cube, sizes
        self.rows = min(rows for rows, _ in shapes)
        units = [
            (a, q, c) for a, (rows, lanes) in enumerate(shapes) for c in range(lanes // LANES) for q in range(rows // self.rows)
        ]
        share = -(-len(units) // COLORS)
        self.units = [(i // share, i % share * self.rows, *unit) for i, unit in enumerate(units)]
        self.vec_row = share * self.rows
        self.vec_row += self.vec_row % 2
        self.height = -(-(self.vec_row + (VECS if sizes else 0)) // 16) * 16
        self.pack = 16 // math.gcd(self.rows, 16)

    @property
    def block(self):
        return (COLORS, self.height, LANES)

    @property
    def buffer(self):
        return (2, COLORS, self.cube.slots, self.height, LANES)

    def runs(self):
        return [(i, i + 1 if i % 4 == 3 else i + 3, self.sizes[i]) for i in (0, 3, 4, 7)]

    def pack_own(self, layer, weights, vectors, temp, store):
        for color, row, a, q, c in self.units:
            lanes = slice(c * LANES, (c + 1) * LANES)
            store(color, row, row + self.rows, weights[a][layer, q * self.rows : (q + 1) * self.rows, lanes])
        if self.sizes:
            for i, vector in enumerate(vectors):
                temp[i : i + 1, : vector.shape[1]] = vector[layer : layer + 1, :].astype(F32)
            store(0, self.vec_row, self.vec_row + VECS, temp[...].astype(BF))

    def place(self, color, first, i):
        return self.cube.place(color, first + i)

    def spread(self, buf, targets, vec):
        merged = self.rows % 4 == 0

        def natural(g, _):
            first = g * self.pack
            for a, target in enumerate(targets):
                rows = target.shape[0] // self.cube.devices
                pieces = rows // self.rows
                count = self.pack
                by_lane = {}
                for color, row, b, q, c in self.units:
                    if b == a:
                        by_lane.setdefault(c, {})[q] = (color, row)
                for c, places in by_lane.items():
                    parts = []
                    for i in range(count):
                        for q in range(pieces):
                            color, row = places[q]
                            part = buf[self.place(color, first, i) + (slice(row, row + self.rows), slice(None))]
                            parts.append(part if merged else part.astype(F32))
                    value = jnp.concatenate(parts, axis=0).astype(target.dtype)
                    height = count * rows
                    target[pl.ds(pl.multiple_of(g * height, 16), height), c * LANES : (c + 1) * LANES] = value
            return 0

        lax.fori_loop(0, self.cube.devices // self.pack, natural, 0)
        for d in range(self.cube.devices if self.sizes else 0):
            value = buf[self.place(0, d, 0) + (slice(self.vec_row, self.vec_row + VECS), slice(None))].astype(F32)
            for lo, hi, size in self.runs():
                vec[lo:hi, d * size : (d + 1) * size] = value[lo:hi, :size]

    def split(self, sources, vec, temp, buf):
        merged = self.rows % 4 == 0

        def natural(g, _):
            first = g * self.pack
            for color, row, a, q, c in self.units:
                rows = sources[a].shape[0] // self.cube.devices
                height = self.pack * rows
                value = sources[a][pl.ds(pl.multiple_of(g * height, 16), height), c * LANES : (c + 1) * LANES]
                if not merged:
                    value = value.astype(F32)
                for i in range(self.pack):
                    lo = i * rows + q * self.rows
                    buf[self.place(color, first, i) + (slice(row, row + self.rows), slice(None))] = value[lo : lo + self.rows].astype(BF)
            return 0

        lax.fori_loop(0, self.cube.devices // self.pack, natural, 0)
        for d in range(self.cube.devices if self.sizes else 0):
            for lo, hi, size in self.runs():
                temp[lo:hi, :size] = vec[lo:hi, d * size : (d + 1) * size]
            buf[self.place(0, d, 0) + (slice(self.vec_row, self.vec_row + VECS), slice(None))] = temp[...].astype(BF)

    def emit(self, layer, block, weights, vectors):
        for color, row, a, q, c in self.units:
            lanes = slice(c * LANES, (c + 1) * LANES)
            weights[a][layer, q * self.rows : (q + 1) * self.rows, lanes] = block[color, row : row + self.rows, :]
        for i, vector in enumerate(vectors):
            vector[layer : layer + 1, :] = block[0, self.vec_row + i : self.vec_row + i + 1, : vector.shape[1]]


class Gather:
    def __init__(self, group, position, source, buf, send, recv):
        self.cube, self.group = group.cube, group
        self.mine, self.core, self.partners, self.other = position
        self.source, self.buf, self.send, self.recv = source, buf, send, recv
        self.ticks = self.cube.bits + 2

    @staticmethod
    def semaphores(cube):
        return (COLORS * cube.bits + 1,)

    def copy(self, color, step):
        cube = self.cube
        if step == cube.bits:
            key, partner = COLORS * cube.bits, self.other
            src = dst = self.buf.at[self.core]
        else:
            key, partner = color * cube.bits + step, self.partners[cube.order(color, step)]
            dst = self.buf.at[self.core, color, pl.ds(cube.flat(color, self.mine, step), 1 << step)]
            src = self.source.at[pl.ds(color, 1)] if step == 0 else dst
        return pltpu.make_async_remote_copy(
            src_ref=src,
            dst_ref=dst,
            send_sem=self.send.at[key],
            recv_sem=self.recv.at[key],
            device_id=(partner,),
            device_id_type=MESH_ID,
        )

    def local(self, sem):
        return [
            pltpu.make_async_copy(
                self.source.at[pl.ds(c, 1)], self.buf.at[self.core, c, pl.ds(self.cube.flat(c, self.mine), 1)], sem.at[c]
            )
            for c in range(COLORS)
        ]

    def tick(self, t):
        bits = self.cube.bits
        for color in range(COLORS):
            if 0 < t <= bits:
                self.copy(color, t - 1).wait_recv()
            if t < bits:
                self.copy(color, t).start()
        if t == bits:
            self.copy(0, bits).start()
        if t > bits:
            self.copy(0, bits).wait()
            for color in range(COLORS):
                for step in range(bits):
                    self.copy(color, step).wait_send()


class Scatter:
    def __init__(self, group, position, blocks, inbox, out, send, recv):
        self.cube = group.cube
        self.mine, self.core, self.partners, self.other = position
        self.blocks, self.inbox, self.out, self.send, self.recv = blocks, inbox, out, send, recv
        self.ticks = self.cube.bits + 2

    @staticmethod
    def semaphores(cube):
        return (COLORS * cube.bits + 1,)

    def copy(self, color, step):
        cube = self.cube
        if step == cube.bits:
            key, partner = COLORS * cube.bits, self.other
            src, dst = self.blocks.at[1 - self.core], self.inbox.at[0]
        else:
            key, partner = color * cube.bits + step, self.partners[cube.order(color, step)]
            size = 1 << step
            start = cube.flat(color, self.mine, step) + (1 - 2 * self.mine[cube.order(color, step)]) * size
            src = self.blocks.at[self.core, color, pl.ds(start, size)]
            dst = self.inbox.at[1, color, pl.ds(size, size)]
        return pltpu.make_async_remote_copy(
            src_ref=src,
            dst_ref=dst,
            send_sem=self.send.at[key],
            recv_sem=self.recv.at[key],
            device_id=(partner,),
            device_id_type=MESH_ID,
        )

    def absorb(self, color, step):
        cube = self.cube
        if step == cube.bits:
            start, size, base, box = 0, cube.slots, 0, 0
        else:
            start, size, base, box = cube.flat(color, self.mine, step), 1 << step, 1 << step, 1
        if step == 0:
            self.out[color] = self.blocks[self.core, color, start].astype(F32) + self.inbox[box, color, base].astype(F32)
            return

        def body(j, _):
            at = (self.core, color, start + j)
            self.blocks[at] = self.blocks[at] + self.inbox[box, color, base + j]
            return 0

        lax.fori_loop(0, size, body, 0)

    def tick(self, t):
        bits = self.cube.bits
        if t == 0:
            self.copy(0, bits).start()
            return
        if t == 1:
            self.copy(0, bits).wait_recv()
        for color in range(COLORS):
            if t > 1:
                self.copy(color, bits + 1 - t).wait_recv()
            self.absorb(color, bits + 1 - t)
            if t <= bits:
                self.copy(color, bits - t).start()
        if t == bits + 1:
            self.copy(0, bits).wait_send()
            for color in range(COLORS):
                for step in range(bits):
                    self.copy(color, step).wait_send()


class Rider:
    def __init__(self):
        self.due = {}

    def add(self, step, point, run):
        self.due.setdefault((step, point), []).append(run)

    def at(self, index, point, where=lambda step: True):
        for (step, slot), runs in sorted(self.due.items(), key=lambda item: item[0]):
            if slot == point and where(step):

                @pl.when(index == step)
                def _(runs=runs):
                    for run in runs:
                        run()


def mm(left, right, dims):
    return lax.dot_general(left, right, dims, preferred_element_type=F32)


def norm_stats(hidden):
    centered = hidden - jnp.mean(hidden, axis=-1, keepdims=True)
    inv_std = lax.rsqrt(jnp.mean(centered * centered, axis=-1, keepdims=True) + EPS)
    return centered * inv_std, inv_std


def norm_back(grad_in, normed, inv_std, gain):
    dnorm = grad_in * gain
    return inv_std * (
        dnorm
        - jnp.mean(dnorm, axis=-1, keepdims=True)
        - normed * jnp.mean(dnorm * normed, axis=-1, keepdims=True)
    )


def half_masks():
    lane = lax.broadcasted_iota(jnp.int32, (1, LANES), 1)
    low = (lane < HEAD_DIM).astype(F32).astype(BF)
    return low, 1 - low


class Dims:
    def __init__(self, images, counts, seq, width, ff):
        self.images, self.slots, self.seq, self.width, self.ff = images, images // counts, seq, width, ff
        self.rows = -(-seq // 16) * 16
        self.steps = images // PER_STEP
        self.blk = PER_STEP * self.rows
        self.tot = images * self.rows
        self.flat = images * seq


def vrow(vec_ref, row, width, start=0):
    return vec_ref[row : row + 1, start : start + width]


def image_rows(dims, image):
    return pl.ds(image, dims.seq, stride=dims.images)


def wide_shape(dims):
    return (dims.width // LANES, dims.flat, LANES)


def wide_load(wide, ref):
    for c in range(wide.shape[0]):
        wide[c] = ref[:, c * LANES : (c + 1) * LANES].astype(F32)


def image_get(dims, wide, image):
    return jnp.concatenate([wide[c, image_rows(dims, image), :] for c in range(wide.shape[0])], axis=1)


def image_put(dims, wide, image, value):
    for c in range(wide.shape[0]):
        wide[c, image_rows(dims, image), :] = value[:, c * LANES : (c + 1) * LANES]


def alive(counts, dims, group, slot):
    return jnp.clip(counts[group] - slot, 0, 1).astype(F32)


def fwd_attn_compute(dims, base, vec_ref, wqkv_ref, wproj_ref, outs, scratch):
    n1_ref, inv_ref, qkv_out, e_ref, il_ref, ctx_ref = outs
    stream, qkv_ref = scratch
    width, rows, seq, total = dims.width, dims.rows, dims.seq, dims.blk
    span = pl.ds(base, total)
    h = stream[span, :]
    n1, inv1 = norm_stats(h)
    n1_ref[...] = n1.astype(BF)
    inv_ref[...] = jnp.broadcast_to(inv1, inv_ref.shape)
    attn_in = (n1 * vrow(vec_ref, N1G, width) + vrow(vec_ref, N1B, width)).astype(BF)
    q = (mm(attn_in, wqkv_ref[:, :width], NN) + vrow(vec_ref, BQV, width)).astype(BF) * BF(HEAD_DIM ** -0.5)
    k = mm(attn_in, wqkv_ref[:, width : 2 * width], NN).astype(BF)
    v = (mm(attn_in, wqkv_ref[:, 2 * width :], NN) + vrow(vec_ref, BQV, width, width)).astype(BF)
    for i, part in enumerate((q, k, v)):
        qkv_ref[0:total, i * width : (i + 1) * width] = part
        qkv_out[:, i * width : (i + 1) * width] = part
    low, high = half_masks()
    lane = lax.broadcasted_iota(jnp.int32, (1, KEYS), 1)
    key_mask = jnp.where(lane < seq, 0.0, -1e30).astype(F32)
    lane_low = lax.broadcasted_iota(jnp.int32, (1, LANES), 1) < HEAD_DIM
    ones = jnp.ones((KEYS, LANES), BF)
    for g in range(PER_STEP):
        r0 = g * rows
        for pair in range(width // LANES):
            c0 = pair * LANES
            qp = qkv_ref[r0 : r0 + rows, c0 : c0 + LANES]
            kp = qkv_ref[r0 : r0 + KEYS, width + c0 : width + c0 + LANES]
            vp = qkv_ref[r0 : r0 + KEYS, 2 * width + c0 : 2 * width + c0 + LANES]
            vo = jnp.concatenate([vp, ones], axis=1)
            parts = []
            for half, mask in enumerate((low, high)):
                s = mm(qp * mask, kp, NT) + key_mask
                e = jnp.exp(s - jnp.max(s, axis=-1, keepdims=True)).astype(BF)
                j = 2 * pair + half
                e_ref[r0 : r0 + rows, j * KEYS : (j + 1) * KEYS] = e
                r = mm(e, vo, NN)
                recip = 1.0 / r[:, LANES:]
                parts.append((r[:, :LANES] * recip, recip))
            ctx_ref[r0 : r0 + rows, c0 : c0 + LANES] = jnp.where(lane_low, parts[0][0], parts[1][0]).astype(BF)
            il_ref[r0 : r0 + rows, c0 : c0 + LANES] = jnp.where(lane_low, parts[0][1], parts[1][1])
    stream[span, :] = h + mm(ctx_ref[...], wproj_ref[...], NN) + vrow(vec_ref, BPJ, width)


def fwd_mlp_compute(dims, base, vec_ref, w1_ref, w2_ref, outs, stream):
    n2_ref, inv_ref, act_ref, slope_ref = outs
    width, span = dims.width, pl.ds(base, dims.blk)
    mid = stream[span, :]
    n2, inv2 = norm_stats(mid)
    n2_ref[...] = n2.astype(BF)
    inv_ref[...] = jnp.broadcast_to(inv2, inv_ref.shape)
    mlp_in = (n2 * vrow(vec_ref, N2G, width) + vrow(vec_ref, N2B, width)).astype(BF)
    chunk = 256
    for c in range(0, dims.ff, chunk):
        pre = mm(mlp_in, w1_ref[:, c : c + chunk], NN) + vrow(vec_ref, BF1, chunk, c)
        cdf = 0.5 + 0.5 * lax.erf(pre * 0.7071067811865476)
        act_ref[:, c : c + chunk] = (pre * cdf).astype(BF)
        slope_ref[:, c : c + chunk] = (cdf + pre * jnp.exp(-0.5 * pre * pre) * 0.3989422804014327).astype(BF)
    stream[span, :] = mid + mm(act_ref[...], w2_ref[...], NN) + vrow(vec_ref, BF2, width)


def bwd_mlp_compute(dims, step, poll, vec_ref, w1_ref, w2_ref, saved, scratch, group, blocks):
    n2_ref, inv_ref, act_ref, slope_ref = saved
    stream, thin, act_all, dpre_all, vecs_ref, temp, dw_ref, dw2_ref, _ = scratch
    width, total = dims.width, dims.blk
    gb_all, mlp_all = thin.at[0], thin.at[1]
    span = pl.ds(pl.multiple_of(step * total, 16), total)

    @pl.when(step == 0)
    def _():
        vecs_ref[...] = jnp.zeros_like(vecs_ref)

    gh = stream[span, :]
    gb = gh.astype(BF)
    gb_all[span, :] = gb
    act_all[span, :] = act_ref[...]
    vecs_ref[BF2 : BF2 + 1, :width] += jnp.sum(gh, axis=0, keepdims=True)
    chunk = 256
    for c in range(0, dims.ff, chunk):
        dpre = mm(gb, w2_ref[c : c + chunk, :], NT) * slope_ref[:, c : c + chunk].astype(F32)
        vecs_ref[BF1 : BF1 + 1, c : c + chunk] += jnp.sum(dpre, axis=0, keepdims=True)
        dpre_all[span, c : c + chunk] = dpre.astype(BF)
    poll()
    dmlp = mm(dpre_all[span, :], w1_ref[...], NT)
    n2 = n2_ref[...].astype(F32)
    mlp_all[span, :] = (n2 * vrow(vec_ref, N2G, width) + vrow(vec_ref, N2B, width)).astype(BF)
    vecs_ref[N2G : N2G + 1, :width] += jnp.sum(dmlp * n2, axis=0, keepdims=True)
    vecs_ref[N2B : N2B + 1, :width] += jnp.sum(dmlp, axis=0, keepdims=True)
    gm = gh + norm_back(dmlp, n2, inv_ref[:, 0:1], vrow(vec_ref, N2G, width))
    vecs_ref[BPJ : BPJ + 1, :width] += jnp.sum(gm, axis=0, keepdims=True)
    stream[span, :] = gm

    @pl.when(step == dims.steps - 1)
    def _():
        for c in range(0, dims.ff, 512):
            dw_ref[:, c : c + 512] = mm(mlp_all[...], dpre_all[:, c : c + 512], TN).astype(BF)
            dw2_ref[c : c + 512, :] = mm(act_all[:, c : c + 512], gb_all[...], TN).astype(BF)
        blocks(lambda buf: group.split([dw_ref, dw2_ref], None, temp, buf))


def bwd_attn_compute(dims, step, poll, vec_ref, wqkv_ref, wproj_ref, saved, scratch, group, blocks):
    n1_ref, inv_ref, qkv_in, e_ref, il_ref, ctx_ref = saved
    stream, thin, several, dqkv_all, vecs_ref, temp, dw_ref, _, qkv_ref = scratch
    width, rows, total = dims.width, dims.rows, dims.blk
    gmb_all, ctx_all = thin.at[0], thin.at[1]
    base = pl.multiple_of(step * total, 16)
    span = pl.ds(base, total)
    qkv_ref[0:total, :] = qkv_in[...]
    gm = stream[span, :]
    gmb = gm.astype(BF)
    gmb_all[span, :] = gmb
    ctx_all[span, :] = ctx_ref[...]
    dctx = mm(gmb, wproj_ref[...], NT).astype(BF).astype(F32) * il_ref[...]
    dos_all = dctx.astype(BF)
    doo = dos_all.astype(F32) * ctx_ref[...].astype(F32)
    doo_high = doo.astype(BF)
    doo_low = doo - doo_high.astype(F32)
    lane_low = lax.broadcasted_iota(jnp.int32, (1, LANES), 1) < HEAD_DIM
    low, high = half_masks()
    minus = jnp.full((KEYS, LANES), -1.0, BF)
    for g in range(PER_STEP):
        r0 = g * rows
        rr = pl.ds(pl.multiple_of(base + r0, 16), rows)
        for pair in range(width // LANES):
            c0 = pair * LANES
            qp = qkv_ref[r0 : r0 + rows, c0 : c0 + LANES]
            kp = qkv_ref[r0 : r0 + KEYS, width + c0 : width + c0 + LANES]
            vp = qkv_ref[r0 : r0 + KEYS, 2 * width + c0 : 2 * width + c0 + LANES]
            vm = jnp.concatenate([vp, minus], axis=1)
            dos = dos_all[r0 : r0 + rows, c0 : c0 + LANES]
            upper = doo_high[r0 : r0 + rows, c0 : c0 + LANES].astype(F32)
            lower = pltpu.roll(doo_low[r0 : r0 + rows, c0 : c0 + LANES], HEAD_DIM, 1)
            dots = [jnp.where(lane_low, a, b).astype(BF) for a, b in ((upper, lower), (lower, upper))]
            dq = dk = dv = None
            for half, mask in enumerate((low, high)):
                j = 2 * pair + half
                e = e_ref[r0 : r0 + rows, j * KEYS : (j + 1) * KEYS]
                dd = mm(jnp.concatenate([dos * mask, dots[half]], axis=1), vm, NT)
                ds = (e.astype(F32) * dd).astype(BF)
                dv_h = mm(e, dos * mask, TN)
                dk_h = mm(ds, qp * mask, TN)
                dq_h = mm(ds, kp * mask, NN)
                dq = dq_h if dq is None else dq + dq_h
                dk = dk_h if dk is None else dk + dk_h
                dv = dv_h if dv is None else dv + dv_h
            dq = dq * (HEAD_DIM ** -0.5)
            dv = dv[:rows]
            vecs_ref[BQV : BQV + 1, c0 : c0 + LANES] += jnp.sum(dq, axis=0, keepdims=True)
            vecs_ref[BQV : BQV + 1, width + c0 : width + c0 + LANES] += jnp.sum(dv, axis=0, keepdims=True)
            dqkv_all[rr, c0 : c0 + LANES] = dq.astype(BF)
            dqkv_all[rr, width + c0 : width + c0 + LANES] = dk[:rows].astype(BF)
            dqkv_all[rr, 2 * width + c0 : 2 * width + c0 + LANES] = dv.astype(BF)
    poll()
    dai = mm(dqkv_all[span, : 3 * width], wqkv_ref[...], NT)
    n1 = n1_ref[...].astype(F32)
    several[span, :width] = (n1 * vrow(vec_ref, N1G, width) + vrow(vec_ref, N1B, width)).astype(BF)
    vecs_ref[N1G : N1G + 1, :width] += jnp.sum(dai * n1, axis=0, keepdims=True)
    vecs_ref[N1B : N1B + 1, :width] += jnp.sum(dai, axis=0, keepdims=True)
    stream[span, :] = gm + norm_back(dai, n1, inv_ref[:, 0:1], vrow(vec_ref, N1G, width))

    @pl.when(step == dims.steps - 1)
    def _():
        for c in range(0, 3 * width, width):
            dw_ref[:, c : c + width] = mm(several[:, :width], dqkv_all[:, c : c + width], TN).astype(BF)
        dw_ref[:, 3 * width : 4 * width] = mm(ctx_all[...], gmb_all[...], TN).astype(BF)
        blocks(lambda buf: group.split([dw_ref.at[:, : 3 * width], dw_ref.at[:, 3 * width : 4 * width]], vecs_ref, temp, buf))


ANY = pl.BlockSpec(memory_space=pl.ANY)
VM = pl.BlockSpec(memory_space=pltpu.VMEM)
SM = pl.BlockSpec(memory_space=pltpu.SMEM)
SDS = jax.ShapeDtypeStruct
DMA = pltpu.SemaphoreType.DMA


def full(shape):
    return pl.BlockSpec(shape, lambda i: (0,) * len(shape), pipeline_mode=pl.Buffered(1))


def take(refs, *counts):
    refs, parts = list(refs), []
    for count in counts:
        parts.append(refs[:count])
        refs = refs[count:]
    assert not refs
    return parts


def params_of(collective=None):
    extra = {} if collective is None else {"collective_id": collective, "has_side_effects": True}
    return pltpu.CompilerParams(vmem_limit_bytes=VMEM_LIMIT, **extra)


def weight_shapes(dims):
    return [(dims.width, 3 * dims.width), (dims.width, dims.width), (dims.width, dims.ff), (dims.ff, dims.width)]


def forward(cube, dims, groups, live, x, params):
    steps, width, ff, tot = dims.steps, dims.width, dims.ff, dims.tot
    shapes = weight_shapes(dims)
    jobs = [(layer, half) for layer in range(LAYERS) for half in (ATTN, MLP)]
    heads = (width // HEAD_DIM) * KEYS
    saved_attn = [(width, BF), (LANES, F32), (3 * width, BF), (heads, BF), (width, F32), (width, BF)]
    saved_mlp = [(width, BF), (LANES, F32), (ff, BF), (ff, BF)]
    last = 2 * LAYERS * steps - 1

    def body(*refs):
        (live_ref, x_ref), args, (wide,), whole, attn_outs, mlp_outs, scratch, gathers = take(
            refs, 2, 12, 1, 5, len(saved_attn), len(saved_mlp), 10, 4 * len(jobs)
        )
        (n1g, n1b, wqkv, bqv, wproj, bpj, n2g, n2b, w1, bf1, w2, bf2) = args
        temp, local_sem, out_sem, stream, qkv_ref, *kept = scratch
        vec_s, wqkv_s, wproj_s, w1_s, w2_s = kept
        index = pl.program_id(0)
        layer, half, step = index // (2 * steps), (index // steps) % 2, index % steps
        base = pl.multiple_of(step * dims.blk, 16)
        position = cube.position()
        weights = ([wqkv, wproj], [w1, w2])
        vectors = ((n1g, n1b, bpj, bqv, n2g, n2b, bf2, bf1), ())
        works = []
        for n, (job_layer, job_half) in enumerate(jobs):
            own, buf, send, recv = gathers[4 * n : 4 * n + 4]
            works.append(Gather(groups[job_half], position, own, buf, send, recv))
        ticks = works[0].ticks

        def pack(n):
            job_layer, job_half = jobs[n]
            own = gathers[4 * n]

            def store(color, lo, hi, value):
                own[color, lo:hi, :] = value

            own[...] = jnp.zeros_like(own)
            groups[job_half].pack_own(job_layer, weights[job_half], vectors[job_half], temp, store)

        def stage(t):
            for n, work in enumerate(works):
                if 0 <= t - n < ticks:
                    if t == n:
                        for copy in work.local(local_sem.at[n]):
                            copy.start()
                    if t - n == 1:
                        for copy in work.local(local_sem.at[n]):
                            copy.wait()
                    work.tick(t - n)

        def saves(n):
            job_layer, job_half = jobs[n]
            which = (1, 2, 0) if job_half == ATTN else (3, 4)
            return [
                pltpu.make_async_copy(kept[k].at[job_layer], whole[k].at[job_layer], out_sem.at[job_layer, k]) for k in which
            ]

        def finish(n):
            job_layer, job_half = jobs[n]
            targets = [wqkv_s, wproj_s] if job_half == ATTN else [w1_s, w2_s]
            if job_half == ATTN:
                vec_s[job_layer] = jnp.zeros(vec_s.shape[1:], F32)
            groups[job_half].spread(gathers[4 * n + 1], [t.at[job_layer] for t in targets], vec_s.at[job_layer])
            for copy in saves(n):
                copy.start()

        def begin():
            temp[...] = jnp.zeros_like(temp)
            pack(0)
            greet(position[2] + [position[3]])
            for t in range(ticks):
                if 0 < t < len(jobs):
                    pack(t)
                stage(t)
                if t == 2:
                    qkv_ref[dims.blk :, :] = jnp.zeros_like(qkv_ref[dims.blk :, :])
                    stream[...] = jnp.zeros_like(stream)
                    wide_load(wide, x_ref)
                    for image in range(dims.images):
                        stream[image * dims.rows : image * dims.rows + dims.seq, :] = image_get(dims, wide, image)
            finish(0)

        rider = Rider()
        rider.add(0, 0, begin)
        for late in range(1, len(jobs)):
            rider.add(min(late, steps - 1), 0, lambda late=late: stage(ticks + late - 1))
        for n in range(1, len(jobs)):
            rider.add(n * steps, 0, lambda n=n: finish(n))
        rider.at(index, 0)

        @pl.when(half == ATTN)
        def _():
            fwd_attn_compute(
                dims, base, vec_s.at[layer], wqkv_s.at[layer], wproj_s.at[layer], attn_outs, (stream, qkv_ref)
            )

        @pl.when(half == MLP)
        def _():
            fwd_mlp_compute(dims, base, vec_s.at[layer], w1_s.at[layer], w2_s.at[layer], mlp_outs, stream)

        @pl.when(index > last - steps)
        def _():
            for g in range(PER_STEP):
                start = pl.multiple_of(base + g * dims.rows, 16)
                group, slot = step * (PER_STEP // dims.slots) + g // dims.slots, g % dims.slots
                image_put(dims, wide, step * PER_STEP + g, stream[pl.ds(start, dims.seq), :] * alive(live_ref, dims, group, slot))

        @pl.when(index == last)
        def _():
            for n in range(len(jobs)):
                for copy in saves(n):
                    copy.wait()

    sem = DMA(Gather.semaphores(cube))
    lead = lambda i: (i // (2 * steps)) * steps
    half_of = lambda i: (i // steps) % 2
    attn_spec = lambda n: pl.BlockSpec((dims.blk, n), lambda i: (lead(i) + (i % steps) * (1 - half_of(i)) + (steps - 1) * half_of(i), 0))
    mlp_spec = lambda n: pl.BlockSpec((dims.blk, n), lambda i: (lead(i) + (i % steps) * half_of(i), 0))
    whole_shapes = [(LAYERS, VECS, ff)] + [(LAYERS,) + s for s in shapes]
    whole_types = [F32, BF, BF, BF, BF]
    outs = pl.pallas_call(
        body,
        grid=(last + 1,),
        in_specs=[SM, full(x.shape)] + [full(p.shape) for p in params],
        out_specs=[full(wide_shape(dims))]
        + [ANY] * 5
        + [attn_spec(n) for n, _ in saved_attn]
        + [mlp_spec(n) for n, _ in saved_mlp],
        out_shape=[SDS(wide_shape(dims), F32)]
        + [SDS(s, t) for s, t in zip(whole_shapes, whole_types)]
        + [SDS((LAYERS * tot, n), t) for n, t in saved_attn + saved_mlp],
        scratch_shapes=[
            pltpu.VMEM((VECS, LANES), F32),
            DMA((len(jobs), COLORS)),
            DMA((LAYERS, 5)),
            pltpu.VMEM((tot, width), F32),
            pltpu.VMEM((dims.blk + KEYS - dims.rows, 3 * width), BF),
        ]
        + [pltpu.VMEM(s, t) for s, t in zip(whole_shapes, whole_types)]
        + sum([[pltpu.VMEM(groups[h].block, BF), pltpu.VMEM(groups[h].buffer, BF), sem, sem] for _, h in jobs], []),
        compiler_params=params_of(0),
        name="forward",
    )(live, x, *params)
    return outs[0], outs[1:6], outs[6:12], outs[12:16]


def spread_ticks(ticks, polls):
    return polls if ticks == len(polls) else [polls[t * len(polls) // ticks] for t in range(ticks)]


def backward(cube, dims, groups, live, grad, whole, saved_attn, saved_mlp):
    steps, width, ff, tot = dims.steps, dims.width, dims.ff, dims.tot
    jobs = [(layer, half) for layer in reversed(range(LAYERS)) for half in (MLP, ATTN)]
    last = len(jobs) * steps - 1

    def body(*refs):
        (live_ref, og_ref), whole_in, attn_in, mlp_in, (wide,), sums, scratch, kept, scatters = take(
            refs, 2, 5, 6, 4, 1, len(jobs), 10, 5, 4 * len(jobs)
        )
        *work_scratch, load_sem = scratch
        stream, qkv_ref = work_scratch[0], work_scratch[8]
        vec_s, wqkv_s, wproj_s, w1_s, w2_s = kept
        index = pl.program_id(0)
        layer, half, step = LAYERS - 1 - index // (2 * steps), 1 - (index // steps) % 2, index % steps
        base = pl.multiple_of(step * dims.blk, 16)
        position = cube.position()
        works = []
        for n, (job_layer, job_half) in enumerate(jobs):
            blocks, inbox, send, recv = scatters[4 * n : 4 * n + 4]
            works.append(Scatter(groups[job_half], position, blocks, inbox, sums[n], send, recv))
        ticks = works[0].ticks

        def loads(n):
            job_layer, job_half = jobs[n]
            which = (1, 2) if job_half == ATTN else (0, 3, 4)
            return [
                pltpu.make_async_copy(whole_in[k].at[job_layer], kept[k].at[job_layer], load_sem.at[job_layer, k]) for k in which
            ]

        def begin():
            for n in range(len(jobs)):
                for copy in loads(n):
                    copy.start()
            qkv_ref[dims.blk :, :] = jnp.zeros_like(qkv_ref[dims.blk :, :])
            stream[...] = jnp.zeros_like(stream)
            wide_load(wide, og_ref)
            for image in range(dims.images):
                stream[image * dims.rows : image * dims.rows + dims.seq, :] = image_get(dims, wide, image) * alive(
                    live_ref, dims, image // dims.slots, image % dims.slots
                )
            greet(position[2] + [position[3]])

        def ready(n):
            for copy in loads(n):
                copy.wait()

        rider = Rider()
        rider.add(0, 0, begin)
        for n in range(len(jobs)):
            rider.add(n * steps, 0, lambda n=n: ready(n))
        end = (last, 2)
        for n, (job_layer, job_half) in enumerate(jobs):
            first = (n + 1) * steps
            if job_half == MLP:
                polls = [(first, 0), (first + 1, 0), (first + 2, 1), (first + 3, 1), (first + 4, 0), (first + 5, 0)]
            else:
                polls = [(first, 0), (first + 1, 0), (first + 2, 1), (first + 3, 1), (first + 4, 0), (first + 5, 0)]
            for t, (at, point) in enumerate(spread_ticks(ticks, polls)):
                if at <= last:
                    rider.add(at, point, lambda n=n, t=t: works[n].tick(t))
                else:
                    rider.add(*end, lambda n=n, t=t: works[n].tick(t))
        left = rider.due.pop(end)
        count = len(left) - ticks
        order = []
        for t in range(ticks):
            order += left[t : t + 1] if t < count else []
            order.append(left[count + t])
        rider.due[end] = order
        rider.at(index, 0)

        @pl.when(half == MLP)
        def _():
            def blocks(run):
                for n, (job_layer, job_half) in enumerate(jobs):
                    if job_half == MLP:

                        @pl.when(layer == job_layer)
                        def _(n=n):
                            run(scatters[4 * n])

            bwd_mlp_compute(
                dims, step, lambda: rider.at(index, 1, lambda at: (at // steps) % 2 == 0), vec_s.at[layer], w1_s.at[layer], w2_s.at[layer],
                mlp_in, work_scratch, groups[MLP], blocks,
            )

        @pl.when(half == ATTN)
        def _():
            def blocks(run):
                for n, (job_layer, job_half) in enumerate(jobs):
                    if job_half == ATTN:

                        @pl.when(layer == job_layer)
                        def _(n=n):
                            run(scatters[4 * n])

            bwd_attn_compute(
                dims, step, lambda: rider.at(index, 1, lambda at: (at // steps) % 2 == 1), vec_s.at[layer], wqkv_s.at[layer], wproj_s.at[layer],
                attn_in, work_scratch, groups[ATTN], blocks,
            )

        @pl.when(index > last - steps)
        def _():
            for g in range(PER_STEP):
                start = pl.multiple_of(base + g * dims.rows, 16)
                image_put(dims, wide, step * PER_STEP + g, stream[pl.ds(start, dims.seq), :])

        rider.at(index, 2)

    sem = DMA(Scatter.semaphores(cube))
    lead = lambda i: (LAYERS - 1 - i // (2 * steps)) * steps
    is_attn = lambda i: (i // steps) % 2
    attn_spec = lambda n: pl.BlockSpec((dims.blk, n), lambda i: (lead(i) + (i % steps) * is_attn(i), 0))
    mlp_spec = lambda n: pl.BlockSpec((dims.blk, n), lambda i: (lead(i) + (i % steps) * (1 - is_attn(i)) + (steps - 1) * is_attn(i), 0))
    whole_shapes = [w.shape for w in whole]
    outs = pl.pallas_call(
        body,
        grid=(last + 1,),
        in_specs=[SM, full(grad.shape)]
        + [ANY] * 5
        + [attn_spec(s.shape[1]) for s in saved_attn]
        + [mlp_spec(s.shape[1]) for s in saved_mlp],
        out_specs=[full(wide_shape(dims))] + [full(groups[h].block) for _, h in jobs],
        out_shape=[SDS(wide_shape(dims), F32)] + [SDS(groups[h].block, F32) for _, h in jobs],
        scratch_shapes=[
            pltpu.VMEM((tot, width), F32),
            pltpu.VMEM((2, tot, width), BF),
            pltpu.VMEM((tot, ff), BF),
            pltpu.VMEM((tot, ff), BF),
            pltpu.VMEM((VECS, ff), F32),
            pltpu.VMEM((VECS, LANES), F32),
            pltpu.VMEM((width, ff), BF),
            pltpu.VMEM((ff, width), BF),
            pltpu.VMEM((dims.blk + KEYS - dims.rows, 3 * width), BF),
            DMA((LAYERS, 5)),
        ]
        + [pltpu.VMEM(w.shape, w.dtype) for w in whole]
        + sum([[pltpu.VMEM(groups[h].buffer, BF), pltpu.VMEM(groups[h].buffer, BF), sem, sem] for _, h in jobs], []),
        compiler_params=params_of(1),
        name="backward",
    )(live, grad, *whole, *saved_attn, *saved_mlp)
    return outs[0], dict(zip(jobs, outs[1:]))


def emit_outputs(dims, groups, hidden, grad, sums, params):
    def body(*refs):
        (hidden_ref, grad_ref), blocks, (out_ref, in_grad_ref), outs = take(refs, 2, 2 * LAYERS, 2, 12)
        (n1g, n1b, wqkv, bqv, wproj, bpj, n2g, n2b, w1, bf1, w2, bf2) = outs
        weights = ([wqkv, wproj], [w1, w2])
        vectors = ((n1g, n1b, bpj, bqv, n2g, n2b, bf2, bf1), ())
        for c in range(hidden_ref.shape[0]):
            lanes = slice(c * LANES, (c + 1) * LANES)
            out_ref[:, lanes] = hidden_ref[c].astype(BF)
            in_grad_ref[:, lanes] = grad_ref[c]
        for layer in range(LAYERS):
            for half in (ATTN, MLP):
                groups[half].emit(layer, blocks[2 * layer + half], weights[half], vectors[half])

    return pl.pallas_call(
        body,
        in_specs=[VM] * (2 + 2 * LAYERS),
        out_specs=[VM] * 14,
        out_shape=[SDS((dims.flat, dims.width), BF), SDS((dims.flat, dims.width), F32)] + [SDS(p.shape, F32) for p in params],
        compiler_params=params_of(),
        name="emit",
    )(hidden, grad, *[sums[layer, half] for layer in range(LAYERS) for half in (ATTN, MLP)])


def per_device(devices, inputs, out_grad, live_counts, *params):
    cube = Cube(devices)
    images, seq, width = inputs.shape
    dims = Dims(images, live_counts.shape[0], seq, width, params[9].shape[1] * devices)
    size = lambda *which: [params[i].shape[1] for i in which]
    groups = [
        Group(cube, [params[2].shape[1:], params[4].shape[1:]], size(0, 1, 5, 3, 6, 7, 11, 9)),
        Group(cube, [params[8].shape[1:], params[10].shape[1:]], []),
    ]
    lay = lambda a: a.transpose(1, 0, 2).reshape(dims.flat, width)
    unlay = lambda a: a.reshape(seq, images, width).transpose(1, 0, 2)
    hidden, whole, saved_attn, saved_mlp = forward(cube, dims, groups, live_counts, lay(inputs), params)
    grad, sums = backward(cube, dims, groups, live_counts, lay(out_grad), whole, saved_attn, saved_mlp)
    outputs, in_grad, *grads = emit_outputs(dims, groups, hidden, grad, sums, params)
    return (unlay(outputs), unlay(in_grad), *grads)


def solution(mesh):
    devices = mesh.shape["fsdp"]
    rows3, flat2, rows2 = P("fsdp", None, None), P(None, "fsdp"), P(None, "fsdp", None)
    param_specs = (flat2, flat2, rows2, flat2, rows2, flat2, flat2, flat2, rows2, flat2, rows2, flat2)
    return jax.shard_map(
        functools.partial(per_device, devices),
        mesh=mesh,
        in_specs=(rows3, rows3, P("fsdp")) + param_specs,
        out_specs=(rows3, rows3) + param_specs,
        check_vma=False,
    )
```

```python
import functools
import math

import jax
import jax.numpy as jnp
from jax import lax
from jax.experimental import pallas as pl
from jax.experimental.pallas import tpu as pltpu
from jax.sharding import PartitionSpec as P

HEAD_DIM = 64
LAYERS = 2
EPS = 1e-06
BF = jnp.bfloat16
F32 = jnp.float32
NN = (((1,), (0,)), ((), ()))
NT = (((1,), (1,)), ((), ()))
TN = (((0,), (0,)), ((), ()))
KEYS = 256
LANES = 128
VMEM_LIMIT = 67_000_000
PER_STEP = 2
MESH_ID = pl.DeviceIdType.MESH
N1G, N1B, BPJ, BQV, N2G, N2B, BF2, BF1 = range(8)
VECS = 8
ATTN, MLP = 0, 1
COLORS = 2


def torus_shape(devices):
    return {16: (4, 2, 2), 64: (4, 4, 4)}.get(devices // 2, (1, 1, devices // 2))


class Cube:
    def __init__(self, devices):
        self.devices = devices
        self.axes = []
        stride = devices
        for extent in torus_shape(devices):
            stride //= extent
            if extent > 1:
                self.axes.append((extent, stride))
        by_axis, self.bits = [], 0
        for extent, _ in self.axes:
            count = extent.bit_length() - 1
            by_axis.append(list(range(self.bits, self.bits + count)))
            self.bits += count
        self.slots = 1 << self.bits
        orders = [by_axis, by_axis[:1] + by_axis[:0:-1]]
        self.orders = [sum(order, []) for order in orders]

    def bits_of(self, device):
        bits = []
        for extent, stride in self.axes:
            pos = (device // stride) % extent
            bits += [pos // 2, (pos + pos // 2) % 2] if extent == 4 else [pos]
        return bits

    def order(self, color, step):
        return self.orders[color][step]

    def flat(self, color, bits, first=0):
        return sum(bits[self.order(color, s)] * (1 << s) for s in range(first, self.bits))

    def place(self, color, device):
        return device % 2, color, self.flat(color, self.bits_of(device))

    def position(self):
        me = lax.axis_index("fsdp")
        partners = []
        for extent, stride in self.axes:
            pos = (me // stride) % extent
            if extent == 4:
                partners += [me + (3 - 2 * pos) * stride, me + (1 - 2 * (pos % 2)) * stride]
            else:
                partners += [me + (1 - 2 * pos) * stride]
        return self.bits_of(me), me % 2, partners, me + 1 - 2 * (me % 2)


def greet(partners):
    barrier = pltpu.get_barrier_semaphore()
    for partner in partners:
        pl.semaphore_signal(barrier, inc=1, device_id=(partner,), device_id_type=MESH_ID)
    pl.semaphore_wait(barrier, len(partners))


class Group:
    def __init__(self, cube, shapes, sizes):
        self.cube, self.sizes = cube, sizes
        self.rows = min(rows for rows, _ in shapes)
        units = [
            (a, q, c) for a, (rows, lanes) in enumerate(shapes) for c in range(lanes // LANES) for q in range(rows // self.rows)
        ]
        share = -(-len(units) // COLORS)
        self.units = [(i // share, i % share * self.rows, *unit) for i, unit in enumerate(units)]
        self.vec_row = share * self.rows
        self.vec_row += self.vec_row % 2
        self.height = -(-(self.vec_row + (VECS if sizes else 0)) // 16) * 16
        self.pack = 16 // math.gcd(self.rows, 16)

    @property
    def block(self):
        return (COLORS, self.height, LANES)

    @property
    def buffer(self):
        return (2, COLORS, self.cube.slots, self.height, LANES)

    def runs(self):
        return [(i, i + 1 if i % 4 == 3 else i + 3, self.sizes[i]) for i in (0, 3, 4, 7)]

    def pack_own(self, layer, weights, vectors, temp, store):
        for color, row, a, q, c in self.units:
            lanes = slice(c * LANES, (c + 1) * LANES)
            span = slice(q * self.rows, (q + 1) * self.rows)
            at = (span, layer, lanes) if weights[a].shape[1] == LAYERS else (layer, span, lanes)
            store(color, row, row + self.rows, weights[a][at])
        if self.sizes:
            for i, vector in enumerate(vectors):
                temp[i : i + 1, : vector.shape[1]] = vector[layer : layer + 1, :].astype(F32)
            store(0, self.vec_row, self.vec_row + VECS, temp[...].astype(BF))

    def place(self, color, first, i):
        return self.cube.place(color, first + i)

    def spread(self, buf, targets, vec):
        merged = self.rows % 4 == 0

        def natural(g, _):
            first = g * self.pack
            for a, target in enumerate(targets):
                rows = target.shape[0] // self.cube.devices
                pieces = rows // self.rows
                count = self.pack
                by_lane = {}
                for color, row, b, q, c in self.units:
                    if b == a:
                        by_lane.setdefault(c, {})[q] = (color, row)
                for c, places in by_lane.items():
                    parts = []
                    for i in range(count):
                        for q in range(pieces):
                            color, row = places[q]
                            part = buf[self.place(color, first, i) + (slice(row, row + self.rows), slice(None))]
                            parts.append(part if merged else part.astype(F32))
                    value = jnp.concatenate(parts, axis=0).astype(target.dtype)
                    height = count * rows
                    target[pl.ds(pl.multiple_of(g * height, 16), height), c * LANES : (c + 1) * LANES] = value
            return 0

        lax.fori_loop(0, self.cube.devices // self.pack, natural, 0)
        for d in range(self.cube.devices if self.sizes else 0):
            value = buf[self.place(0, d, 0) + (slice(self.vec_row, self.vec_row + VECS), slice(None))].astype(F32)
            for lo, hi, size in self.runs():
                vec[lo:hi, d * size : (d + 1) * size] = value[lo:hi, :size]

    def split(self, sources, vec, temp, buf):
        merged = self.rows % 4 == 0

        def natural(g, _):
            first = g * self.pack
            for color, row, a, q, c in self.units:
                rows = sources[a].shape[0] // self.cube.devices
                height = self.pack * rows
                value = sources[a][pl.ds(pl.multiple_of(g * height, 16), height), c * LANES : (c + 1) * LANES]
                if not merged:
                    value = value.astype(F32)
                for i in range(self.pack):
                    lo = i * rows + q * self.rows
                    buf[self.place(color, first, i) + (slice(row, row + self.rows), slice(None))] = value[lo : lo + self.rows].astype(BF)
            return 0

        lax.fori_loop(0, self.cube.devices // self.pack, natural, 0)
        for d in range(self.cube.devices if self.sizes else 0):
            for lo, hi, size in self.runs():
                temp[lo:hi, :size] = vec[lo:hi, d * size : (d + 1) * size]
            buf[self.place(0, d, 0) + (slice(self.vec_row, self.vec_row + VECS), slice(None))] = temp[...].astype(BF)

    def emit(self, layer, block, weights, vectors):
        for color, row, a, q, c in self.units:
            lanes = slice(c * LANES, (c + 1) * LANES)
            span = slice(q * self.rows, (q + 1) * self.rows)
            at = (span, layer, lanes) if weights[a].shape[1] == LAYERS else (layer, span, lanes)
            weights[a][at] = block[color, row : row + self.rows, :]
        for i, vector in enumerate(vectors):
            vector[layer : layer + 1, :] = block[0, self.vec_row + i : self.vec_row + i + 1, : vector.shape[1]]


class Gather:
    def __init__(self, group, position, source, buf, send, recv):
        self.cube, self.group = group.cube, group
        self.mine, self.core, self.partners, self.other = position
        self.source, self.buf, self.send, self.recv = source, buf, send, recv
        self.ticks = self.cube.bits + 2

    @staticmethod
    def semaphores(cube):
        return (COLORS * cube.bits + 1,)

    def copy(self, color, step):
        cube = self.cube
        if step == cube.bits:
            key, partner = COLORS * cube.bits, self.other
            src = dst = self.buf.at[self.core]
        else:
            key, partner = color * cube.bits + step, self.partners[cube.order(color, step)]
            dst = self.buf.at[self.core, color, pl.ds(cube.flat(color, self.mine, step), 1 << step)]
            src = self.source.at[pl.ds(color, 1)] if step == 0 else dst
        return pltpu.make_async_remote_copy(
            src_ref=src,
            dst_ref=dst,
            send_sem=self.send.at[key],
            recv_sem=self.recv.at[key],
            device_id=(partner,),
            device_id_type=MESH_ID,
        )

    def local(self, sem):
        return [
            pltpu.make_async_copy(
                self.source.at[pl.ds(c, 1)], self.buf.at[self.core, c, pl.ds(self.cube.flat(c, self.mine), 1)], sem.at[c]
            )
            for c in range(COLORS)
        ]

    def tick(self, t):
        bits = self.cube.bits
        for color in range(COLORS):
            if 0 < t <= bits:
                self.copy(color, t - 1).wait_recv()
            if t < bits:
                self.copy(color, t).start()
        if t == bits:
            self.copy(0, bits).start()
        if t > bits:
            self.copy(0, bits).wait()
            for color in range(COLORS):
                for step in range(bits):
                    self.copy(color, step).wait_send()


class Scatter:
    def __init__(self, group, position, blocks, inbox, out, send, recv):
        self.cube = group.cube
        self.mine, self.core, self.partners, self.other = position
        self.blocks, self.inbox, self.out, self.send, self.recv = blocks, inbox, out, send, recv
        self.ticks = self.cube.bits + 2

    @staticmethod
    def semaphores(cube):
        return (COLORS * cube.bits + 1,)

    def copy(self, color, step):
        cube = self.cube
        if step == cube.bits:
            key, partner = COLORS * cube.bits, self.other
            src, dst = self.blocks.at[1 - self.core], self.inbox.at[0]
        else:
            key, partner = color * cube.bits + step, self.partners[cube.order(color, step)]
            size = 1 << step
            start = cube.flat(color, self.mine, step) + (1 - 2 * self.mine[cube.order(color, step)]) * size
            src = self.blocks.at[self.core, color, pl.ds(start, size)]
            dst = self.inbox.at[1, color, pl.ds(size, size)]
        return pltpu.make_async_remote_copy(
            src_ref=src,
            dst_ref=dst,
            send_sem=self.send.at[key],
            recv_sem=self.recv.at[key],
            device_id=(partner,),
            device_id_type=MESH_ID,
        )

    def absorb(self, color, step):
        cube = self.cube
        if step == cube.bits:
            start, size, base, box = 0, cube.slots, 0, 0
        else:
            start, size, base, box = cube.flat(color, self.mine, step), 1 << step, 1 << step, 1
        if step == 0:
            self.out[color] = self.blocks[self.core, color, start].astype(F32) + self.inbox[box, color, base].astype(F32)
            return

        def body(j, _):
            at = (self.core, color, start + j)
            self.blocks[at] = self.blocks[at] + self.inbox[box, color, base + j]
            return 0

        lax.fori_loop(0, size, body, 0)

    def tick(self, t):
        bits = self.cube.bits
        if t == 0:
            self.copy(0, bits).start()
            return
        if t == 1:
            self.copy(0, bits).wait_recv()
        for color in range(COLORS):
            if t > 1:
                self.copy(color, bits + 1 - t).wait_recv()
            self.absorb(color, bits + 1 - t)
            if t <= bits:
                self.copy(color, bits - t).start()
        if t == bits + 1:
            self.copy(0, bits).wait_send()
            for color in range(COLORS):
                for step in range(bits):
                    self.copy(color, step).wait_send()


class Rider:
    def __init__(self):
        self.due = {}

    def add(self, step, point, run):
        self.due.setdefault((step, point), []).append(run)

    def at(self, index, point, where=lambda step: True):
        for (step, slot), runs in sorted(self.due.items(), key=lambda item: item[0]):
            if slot == point and where(step):

                @pl.when(index == step)
                def _(runs=runs):
                    for run in runs:
                        run()


def mm(left, right, dims):
    return lax.dot_general(left, right, dims, preferred_element_type=F32)


def norm_stats(hidden):
    centered = hidden - jnp.mean(hidden, axis=-1, keepdims=True)
    inv_std = lax.rsqrt(jnp.mean(centered * centered, axis=-1, keepdims=True) + EPS)
    return centered * inv_std, inv_std


def norm_back(grad_in, normed, inv_std, gain):
    dnorm = grad_in * gain
    return inv_std * (
        dnorm
        - jnp.mean(dnorm, axis=-1, keepdims=True)
        - normed * jnp.mean(dnorm * normed, axis=-1, keepdims=True)
    )


def half_masks():
    lane = lax.broadcasted_iota(jnp.int32, (1, LANES), 1)
    low = (lane < HEAD_DIM).astype(F32).astype(BF)
    return low, 1 - low


class Dims:
    def __init__(self, images, counts, seq, width, ff):
        self.images, self.slots, self.seq, self.width, self.ff = images, images // counts, seq, width, ff
        self.rows = -(-seq // 16) * 16
        self.steps = images // PER_STEP
        self.blk = PER_STEP * self.rows
        self.tot = images * self.rows
        self.flat = images * seq


def vrow(vec_ref, row, width, start=0):
    return vec_ref[row : row + 1, start : start + width]


def image_rows(dims, image):
    return pl.ds(image, dims.seq, stride=dims.images)


def wide_shape(dims):
    return (dims.width // LANES, dims.flat, LANES)


def wide_load(wide, ref):
    for c in range(wide.shape[0]):
        wide[c] = ref[:, c * LANES : (c + 1) * LANES].astype(F32)


def image_get(dims, wide, image):
    return jnp.concatenate([wide[c, image_rows(dims, image), :] for c in range(wide.shape[0])], axis=1)


def image_put(dims, wide, image, value):
    for c in range(wide.shape[0]):
        wide[c, image_rows(dims, image), :] = value[:, c * LANES : (c + 1) * LANES]


def alive(counts, dims, group, slot):
    return jnp.clip(counts[group] - slot, 0, 1).astype(F32)


def fwd_attn_compute(dims, base, vec_ref, wqkv_ref, wproj_ref, outs, scratch):
    n1_ref, inv_ref, qkv_out, e_ref, il_ref, ctx_ref = outs
    stream, qkv_ref = scratch
    width, rows, seq, total = dims.width, dims.rows, dims.seq, dims.blk
    span = pl.ds(base, total)
    h = stream[span, :]
    n1, inv1 = norm_stats(h)
    n1_ref[...] = n1.astype(BF)
    inv_ref[...] = jnp.broadcast_to(inv1, inv_ref.shape)
    attn_in = (n1 * vrow(vec_ref, N1G, width) + vrow(vec_ref, N1B, width)).astype(BF)
    q = (mm(attn_in, wqkv_ref[:, :width], NN) + vrow(vec_ref, BQV, width)).astype(BF) * BF(HEAD_DIM ** -0.5)
    k = mm(attn_in, wqkv_ref[:, width : 2 * width], NN).astype(BF)
    v = (mm(attn_in, wqkv_ref[:, 2 * width :], NN) + vrow(vec_ref, BQV, width, width)).astype(BF)
    for i, part in enumerate((q, k, v)):
        qkv_ref[0:total, i * width : (i + 1) * width] = part
        qkv_out[:, i * width : (i + 1) * width] = part
    low, high = half_masks()
    lane = lax.broadcasted_iota(jnp.int32, (1, KEYS), 1)
    key_mask = jnp.where(lane < seq, 0.0, -1e30).astype(F32)
    lane_low = lax.broadcasted_iota(jnp.int32, (1, LANES), 1) < HEAD_DIM
    ones = jnp.ones((KEYS, LANES), BF)
    for g in range(PER_STEP):
        r0 = g * rows
        for pair in range(width // LANES):
            c0 = pair * LANES
            qp = qkv_ref[r0 : r0 + rows, c0 : c0 + LANES]
            kp = qkv_ref[r0 : r0 + KEYS, width + c0 : width + c0 + LANES]
            vp = qkv_ref[r0 : r0 + KEYS, 2 * width + c0 : 2 * width + c0 + LANES]
            vo = jnp.concatenate([vp, ones], axis=1)
            parts = []
            for half, mask in enumerate((low, high)):
                s = mm(qp * mask, kp, NT) + key_mask
                e = jnp.exp(s - jnp.max(s, axis=-1, keepdims=True)).astype(BF)
                j = 2 * pair + half
                e_ref[r0 : r0 + rows, j * KEYS : (j + 1) * KEYS] = e
                r = mm(e, vo, NN)
                recip = 1.0 / r[:, LANES:]
                parts.append((r[:, :LANES] * recip, recip))
            ctx_ref[r0 : r0 + rows, c0 : c0 + LANES] = jnp.where(lane_low, parts[0][0], parts[1][0]).astype(BF)
            il_ref[r0 : r0 + rows, c0 : c0 + LANES] = jnp.where(lane_low, parts[0][1], parts[1][1])
    stream[span, :] = h + mm(ctx_ref[...], wproj_ref[...], NN) + vrow(vec_ref, BPJ, width)


def fwd_mlp_compute(dims, base, vec_ref, w1_ref, w2_ref, outs, stream):
    n2_ref, inv_ref, act_ref, slope_ref = outs
    width, span = dims.width, pl.ds(base, dims.blk)
    mid = stream[span, :]
    n2, inv2 = norm_stats(mid)
    n2_ref[...] = n2.astype(BF)
    inv_ref[...] = jnp.broadcast_to(inv2, inv_ref.shape)
    mlp_in = (n2 * vrow(vec_ref, N2G, width) + vrow(vec_ref, N2B, width)).astype(BF)
    chunk = 256
    for c in range(0, dims.ff, chunk):
        pre = mm(mlp_in, w1_ref[:, c : c + chunk], NN) + vrow(vec_ref, BF1, chunk, c)
        cdf = 0.5 + 0.5 * lax.erf(pre * 0.7071067811865476)
        act_ref[:, c : c + chunk] = (pre * cdf).astype(BF)
        slope_ref[:, c : c + chunk] = (cdf + pre * jnp.exp(-0.5 * pre * pre) * 0.3989422804014327).astype(BF)
    stream[span, :] = mid + mm(act_ref[...], w2_ref[...], NN) + vrow(vec_ref, BF2, width)


def bwd_mlp_compute(dims, step, poll, vec_ref, w1_ref, w2_ref, saved, scratch, group, blocks):
    n2_ref, inv_ref, act_ref, slope_ref = saved
    stream, thin, act_all, dpre_all, vecs_ref, temp, dw_ref, dw2_ref, _ = scratch
    width, total = dims.width, dims.blk
    gb_all, mlp_all = thin.at[0], thin.at[1]
    span = pl.ds(pl.multiple_of(step * total, 16), total)

    @pl.when(step == 0)
    def _():
        vecs_ref[...] = jnp.zeros_like(vecs_ref)

    gh = stream[span, :]
    gb = gh.astype(BF)
    gb_all[span, :] = gb
    act_all[span, :] = act_ref[...]
    vecs_ref[BF2 : BF2 + 1, :width] += jnp.sum(gh, axis=0, keepdims=True)
    chunk = 256
    for c in range(0, dims.ff, chunk):
        dpre = mm(gb, w2_ref[c : c + chunk, :], NT) * slope_ref[:, c : c + chunk].astype(F32)
        vecs_ref[BF1 : BF1 + 1, c : c + chunk] += jnp.sum(dpre, axis=0, keepdims=True)
        dpre_all[span, c : c + chunk] = dpre.astype(BF)
    poll()
    dmlp = mm(dpre_all[span, :], w1_ref[...], NT)
    n2 = n2_ref[...].astype(F32)
    mlp_all[span, :] = (n2 * vrow(vec_ref, N2G, width) + vrow(vec_ref, N2B, width)).astype(BF)
    vecs_ref[N2G : N2G + 1, :width] += jnp.sum(dmlp * n2, axis=0, keepdims=True)
    vecs_ref[N2B : N2B + 1, :width] += jnp.sum(dmlp, axis=0, keepdims=True)
    gm = gh + norm_back(dmlp, n2, inv_ref[:, 0:1], vrow(vec_ref, N2G, width))
    vecs_ref[BPJ : BPJ + 1, :width] += jnp.sum(gm, axis=0, keepdims=True)
    stream[span, :] = gm

    @pl.when(step == dims.steps - 1)
    def _():
        for c in range(0, dims.ff, 512):
            dw_ref[:, c : c + 512] = mm(mlp_all[...], dpre_all[:, c : c + 512], TN).astype(BF)
            dw2_ref[c : c + 512, :] = mm(act_all[:, c : c + 512], gb_all[...], TN).astype(BF)
        blocks(lambda buf: group.split([dw_ref, dw2_ref], None, temp, buf))


def bwd_attn_compute(dims, step, poll, vec_ref, wqkv_ref, wproj_ref, saved, scratch, group, blocks):
    n1_ref, inv_ref, qkv_in, e_ref, il_ref, ctx_ref = saved
    stream, thin, several, dqkv_all, vecs_ref, temp, dw_ref, _, qkv_ref = scratch
    width, rows, total = dims.width, dims.rows, dims.blk
    gmb_all, ctx_all = thin.at[0], thin.at[1]
    base = pl.multiple_of(step * total, 16)
    span = pl.ds(base, total)
    qkv_ref[0:total, :] = qkv_in[...]
    gm = stream[span, :]
    gmb = gm.astype(BF)
    gmb_all[span, :] = gmb
    ctx_all[span, :] = ctx_ref[...]
    dctx = mm(gmb, wproj_ref[...], NT).astype(BF).astype(F32) * il_ref[...]
    dos_all = dctx.astype(BF)
    doo = dos_all.astype(F32) * ctx_ref[...].astype(F32)
    doo_high = doo.astype(BF)
    doo_low = doo - doo_high.astype(F32)
    lane_low = lax.broadcasted_iota(jnp.int32, (1, LANES), 1) < HEAD_DIM
    low, high = half_masks()
    minus = jnp.full((KEYS, LANES), -1.0, BF)
    for g in range(PER_STEP):
        r0 = g * rows
        rr = pl.ds(pl.multiple_of(base + r0, 16), rows)
        for pair in range(width // LANES):
            c0 = pair * LANES
            qp = qkv_ref[r0 : r0 + rows, c0 : c0 + LANES]
            kp = qkv_ref[r0 : r0 + KEYS, width + c0 : width + c0 + LANES]
            vp = qkv_ref[r0 : r0 + KEYS, 2 * width + c0 : 2 * width + c0 + LANES]
            vm = jnp.concatenate([vp, minus], axis=1)
            dos = dos_all[r0 : r0 + rows, c0 : c0 + LANES]
            upper = doo_high[r0 : r0 + rows, c0 : c0 + LANES].astype(F32)
            lower = pltpu.roll(doo_low[r0 : r0 + rows, c0 : c0 + LANES], HEAD_DIM, 1)
            dots = [jnp.where(lane_low, a, b).astype(BF) for a, b in ((upper, lower), (lower, upper))]
            dq = dk = dv = None
            for half, mask in enumerate((low, high)):
                j = 2 * pair + half
                e = e_ref[r0 : r0 + rows, j * KEYS : (j + 1) * KEYS]
                dd = mm(jnp.concatenate([dos * mask, dots[half]], axis=1), vm, NT)
                ds = (e.astype(F32) * dd).astype(BF)
                dv_h = mm(e, dos * mask, TN)
                dk_h = mm(ds, qp * mask, TN)
                dq_h = mm(ds, kp * mask, NN)
                dq = dq_h if dq is None else dq + dq_h
                dk = dk_h if dk is None else dk + dk_h
                dv = dv_h if dv is None else dv + dv_h
            dq = dq * (HEAD_DIM ** -0.5)
            dv = dv[:rows]
            vecs_ref[BQV : BQV + 1, c0 : c0 + LANES] += jnp.sum(dq, axis=0, keepdims=True)
            vecs_ref[BQV : BQV + 1, width + c0 : width + c0 + LANES] += jnp.sum(dv, axis=0, keepdims=True)
            dqkv_all[rr, c0 : c0 + LANES] = dq.astype(BF)
            dqkv_all[rr, width + c0 : width + c0 + LANES] = dk[:rows].astype(BF)
            dqkv_all[rr, 2 * width + c0 : 2 * width + c0 + LANES] = dv.astype(BF)
    poll()
    dai = mm(dqkv_all[span, : 3 * width], wqkv_ref[...], NT)
    n1 = n1_ref[...].astype(F32)
    several[span, :width] = (n1 * vrow(vec_ref, N1G, width) + vrow(vec_ref, N1B, width)).astype(BF)
    vecs_ref[N1G : N1G + 1, :width] += jnp.sum(dai * n1, axis=0, keepdims=True)
    vecs_ref[N1B : N1B + 1, :width] += jnp.sum(dai, axis=0, keepdims=True)
    stream[span, :] = gm + norm_back(dai, n1, inv_ref[:, 0:1], vrow(vec_ref, N1G, width))

    @pl.when(step == dims.steps - 1)
    def _():
        for c in range(0, 3 * width, width):
            dw_ref[:, c : c + width] = mm(several[:, :width], dqkv_all[:, c : c + width], TN).astype(BF)
        dw_ref[:, 3 * width : 4 * width] = mm(ctx_all[...], gmb_all[...], TN).astype(BF)
        blocks(lambda buf: group.split([dw_ref.at[:, : 3 * width], dw_ref.at[:, 3 * width : 4 * width]], vecs_ref, temp, buf))


ANY = pl.BlockSpec(memory_space=pl.ANY)
VM = pl.BlockSpec(memory_space=pltpu.VMEM)
SM = pl.BlockSpec(memory_space=pltpu.SMEM)
SDS = jax.ShapeDtypeStruct
DMA = pltpu.SemaphoreType.DMA


def full(shape):
    return pl.BlockSpec(shape, lambda i: (0,) * len(shape), pipeline_mode=pl.Buffered(1))


def take(refs, *counts):
    refs, parts = list(refs), []
    for count in counts:
        parts.append(refs[:count])
        refs = refs[count:]
    assert not refs
    return parts


def params_of(collective=None):
    extra = {} if collective is None else {"collective_id": collective, "has_side_effects": True}
    return pltpu.CompilerParams(vmem_limit_bytes=VMEM_LIMIT, **extra)


def weight_shapes(dims):
    return [(dims.width, 3 * dims.width), (dims.width, dims.width), (dims.width, dims.ff), (dims.ff, dims.width)]


def forward(cube, dims, groups, live, x, params):
    steps, width, ff, tot = dims.steps, dims.width, dims.ff, dims.tot
    shapes = weight_shapes(dims)
    jobs = [(layer, half) for layer in range(LAYERS) for half in (ATTN, MLP)]
    heads = (width // HEAD_DIM) * KEYS
    saved_attn = [(width, BF), (LANES, F32), (3 * width, BF), (heads, BF), (width, F32), (width, BF)]
    saved_mlp = [(width, BF), (LANES, F32), (ff, BF), (ff, BF)]
    last = 2 * LAYERS * steps - 1

    def body(*refs):
        (live_ref, x_ref), args, (wide,), whole, attn_outs, mlp_outs, scratch, gathers = take(
            refs, 2, 12, 1, 5, len(saved_attn), len(saved_mlp), 10, 4 * len(jobs)
        )
        (n1g, n1b, wqkv, bqv, wproj, bpj, n2g, n2b, w1, bf1, w2, bf2) = args
        temp, local_sem, out_sem, stream, qkv_ref, *kept = scratch
        vec_s, wqkv_s, wproj_s, w1_s, w2_s = kept
        index = pl.program_id(0)
        layer, half, step = index // (2 * steps), (index // steps) % 2, index % steps
        base = pl.multiple_of(step * dims.blk, 16)
        position = cube.position()
        weights = ([wqkv, wproj], [w1, w2])
        vectors = ((n1g, n1b, bpj, bqv, n2g, n2b, bf2, bf1), ())
        works = []
        for n, (job_layer, job_half) in enumerate(jobs):
            own, buf, send, recv = gathers[4 * n : 4 * n + 4]
            works.append(Gather(groups[job_half], position, own, buf, send, recv))
        ticks = works[0].ticks

        def pack(n):
            job_layer, job_half = jobs[n]
            own = gathers[4 * n]

            def store(color, lo, hi, value):
                own[color, lo:hi, :] = value

            own[...] = jnp.zeros_like(own)
            groups[job_half].pack_own(job_layer, weights[job_half], vectors[job_half], temp, store)

        begins = [0, 2] + [ticks - 1 + 2 * n for n in range(len(jobs) - 2)]

        def tick(n, t):
            if t == 0:
                for copy in works[n].local(local_sem.at[n]):
                    copy.start()
            if t == 1:
                for copy in works[n].local(local_sem.at[n]):
                    copy.wait()
            works[n].tick(t)

        def saves(n):
            job_layer, job_half = jobs[n]
            which = (1, 2, 0) if job_half == ATTN else (3, 4)
            return [
                pltpu.make_async_copy(kept[k].at[job_layer], whole[k].at[job_layer], out_sem.at[job_layer, k]) for k in which
            ]

        def finish(n):
            job_layer, job_half = jobs[n]
            targets = [wqkv_s, wproj_s] if job_half == ATTN else [w1_s, w2_s]
            if job_half == ATTN:
                vec_s[job_layer] = jnp.zeros(vec_s.shape[1:], F32)
            groups[job_half].spread(gathers[4 * n + 1], [t.at[job_layer] for t in targets], vec_s.at[job_layer])
            for copy in saves(n):
                copy.start()

        def begin():
            temp[...] = jnp.zeros_like(temp)
            pack(0)
            greet(position[2] + [position[3]])
            for t in range(ticks):
                for n in range(len(jobs)):
                    if 0 <= t - begins[n] < ticks:
                        tick(n, t - begins[n])
                if t + 1 < len(jobs):
                    pack(t + 1)
                if t == 2:
                    qkv_ref[dims.blk :, :] = jnp.zeros_like(qkv_ref[dims.blk :, :])
                    stream[...] = jnp.zeros_like(stream)
                    wide_load(wide, x_ref)
                    for image in range(dims.images):
                        stream[image * dims.rows : image * dims.rows + dims.seq, :] = image_get(dims, wide, image)
            finish(0)

        rider = Rider()
        rider.add(0, 0, begin)
        timed = [(), (0, 0, 0, 0, 3, 4), (0, 1, 2, 3, 5, 7), (2, 4, 6, 8, 11, 12)]
        for late in range(ticks, begins[-1] + ticks):
            at = late - ticks + 1
            at += at // steps
            for n in range(1, len(jobs)):
                if 0 <= late - begins[n] < ticks:
                    t = late - begins[n]
                    poll = timed[n][t] if ticks == 6 and steps == 4 and n < len(timed) else at
                    rider.add(min(poll, n * steps), 0, lambda n=n, t=t: tick(n, t))
        for n in range(1, len(jobs)):
            rider.add(n * steps, 0, lambda n=n: finish(n))
        rider.at(index, 0)

        @pl.when(half == ATTN)
        def _():
            fwd_attn_compute(
                dims, base, vec_s.at[layer], wqkv_s.at[layer], wproj_s.at[layer], attn_outs, (stream, qkv_ref)
            )

        @pl.when(half == MLP)
        def _():
            fwd_mlp_compute(dims, base, vec_s.at[layer], w1_s.at[layer], w2_s.at[layer], mlp_outs, stream)

        @pl.when(index > last - steps)
        def _():
            for g in range(PER_STEP):
                start = pl.multiple_of(base + g * dims.rows, 16)
                group, slot = step * (PER_STEP // dims.slots) + g // dims.slots, g % dims.slots
                image_put(dims, wide, step * PER_STEP + g, stream[pl.ds(start, dims.seq), :] * alive(live_ref, dims, group, slot))

        @pl.when(index == last)
        def _():
            for n in range(len(jobs)):
                for copy in saves(n):
                    copy.wait()

    sem = DMA(Gather.semaphores(cube))
    lead = lambda i: (i // (2 * steps)) * steps
    half_of = lambda i: (i // steps) % 2
    attn_spec = lambda n: pl.BlockSpec((dims.blk, n), lambda i: (lead(i) + (i % steps) * (1 - half_of(i)) + (steps - 1) * half_of(i), 0))
    mlp_spec = lambda n: pl.BlockSpec((dims.blk, n), lambda i: (lead(i) + (i % steps) * half_of(i), 0))
    whole_shapes = [(LAYERS, VECS, ff)] + [(LAYERS,) + s for s in shapes]
    whole_types = [F32, BF, BF, BF, BF]
    outs = pl.pallas_call(
        body,
        grid=(last + 1,),
        in_specs=[SM, full(x.shape)] + [full(p.shape) for p in params],
        out_specs=[full(wide_shape(dims))]
        + [ANY] * 5
        + [attn_spec(n) for n, _ in saved_attn]
        + [mlp_spec(n) for n, _ in saved_mlp],
        out_shape=[SDS(wide_shape(dims), F32)]
        + [SDS(s, t) for s, t in zip(whole_shapes, whole_types)]
        + [SDS((LAYERS * tot, n), t) for n, t in saved_attn + saved_mlp],
        scratch_shapes=[
            pltpu.VMEM((VECS, LANES), F32),
            DMA((len(jobs), COLORS)),
            DMA((LAYERS, 5)),
            pltpu.VMEM((tot, width), F32),
            pltpu.VMEM((dims.blk + KEYS - dims.rows, 3 * width), BF),
        ]
        + [pltpu.VMEM(s, t) for s, t in zip(whole_shapes, whole_types)]
        + sum([[pltpu.VMEM(groups[h].block, BF), pltpu.VMEM(groups[h].buffer, BF), sem, sem] for _, h in jobs], []),
        compiler_params=params_of(0),
        name="forward",
    )(live, x, *params)
    return outs[0], outs[1:6], outs[6:12], outs[12:16]


def spread_ticks(ticks, polls):
    return polls if ticks == len(polls) else [polls[t * len(polls) // ticks] for t in range(ticks)]


def backward(cube, dims, groups, live, grad, whole, saved_attn, saved_mlp):
    steps, width, ff, tot = dims.steps, dims.width, dims.ff, dims.tot
    jobs = [(layer, half) for layer in reversed(range(LAYERS)) for half in (MLP, ATTN)]
    last = len(jobs) * steps - 1

    def body(*refs):
        (live_ref, og_ref), whole_in, attn_in, mlp_in, (wide,), sums, scratch, kept, scatters = take(
            refs, 2, 5, 6, 4, 1, len(jobs), 10, 5, 4 * len(jobs)
        )
        *work_scratch, load_sem = scratch
        stream, qkv_ref = work_scratch[0], work_scratch[8]
        vec_s, wqkv_s, wproj_s, w1_s, w2_s = kept
        index = pl.program_id(0)
        layer, half, step = LAYERS - 1 - index // (2 * steps), 1 - (index // steps) % 2, index % steps
        base = pl.multiple_of(step * dims.blk, 16)
        position = cube.position()
        works = []
        for n, (job_layer, job_half) in enumerate(jobs):
            blocks, inbox, send, recv = scatters[4 * n : 4 * n + 4]
            works.append(Scatter(groups[job_half], position, blocks, inbox, sums[n], send, recv))
        ticks = works[0].ticks

        def loads(n):
            job_layer, job_half = jobs[n]
            which = (1, 2) if job_half == ATTN else (0, 3, 4)
            return [
                pltpu.make_async_copy(whole_in[k].at[job_layer], kept[k].at[job_layer], load_sem.at[job_layer, k]) for k in which
            ]

        def begin():
            for n in range(len(jobs)):
                for copy in loads(n):
                    copy.start()
            qkv_ref[dims.blk :, :] = jnp.zeros_like(qkv_ref[dims.blk :, :])
            stream[...] = jnp.zeros_like(stream)
            wide_load(wide, og_ref)
            for image in range(dims.images):
                stream[image * dims.rows : image * dims.rows + dims.seq, :] = image_get(dims, wide, image) * alive(
                    live_ref, dims, image // dims.slots, image % dims.slots
                )
            greet(position[2] + [position[3]])

        def ready(n):
            for copy in loads(n):
                copy.wait()

        rider = Rider()
        rider.add(0, 0, begin)
        for n in range(len(jobs)):
            rider.add(n * steps, 0, lambda n=n: ready(n))
        end = (last, 2)
        for n, (job_layer, job_half) in enumerate(jobs):
            first = (n + 1) * steps
            if job_half == MLP:
                polls = [(first, 0), (first + 1, 0), (first + 2, 1), (first + 3, 1), (first + 4, 0), (first + 5, 0)]
            else:
                polls = [(first, 0), (first + 1, 0), (first + 2, 1), (first + 3, 1), (first + 4, 0), (first + 5, 0)]
            for t, (at, point) in enumerate(spread_ticks(ticks, polls)):
                if at <= last:
                    rider.add(at, point, lambda n=n, t=t: works[n].tick(t))
                else:
                    rider.add(*end, lambda n=n, t=t: works[n].tick(t))
        left = rider.due.pop(end)
        count = len(left) - ticks
        order = []
        for t in range(ticks):
            order += left[t : t + 1] if t < count else []
            order.append(left[count + t])
        rider.due[end] = order
        rider.at(index, 0)

        @pl.when(half == MLP)
        def _():
            def blocks(run):
                for n, (job_layer, job_half) in enumerate(jobs):
                    if job_half == MLP:

                        @pl.when(layer == job_layer)
                        def _(n=n):
                            run(scatters[4 * n])

            bwd_mlp_compute(
                dims, step, lambda: rider.at(index, 1, lambda at: (at // steps) % 2 == 0), vec_s.at[layer], w1_s.at[layer], w2_s.at[layer],
                mlp_in, work_scratch, groups[MLP], blocks,
            )

        @pl.when(half == ATTN)
        def _():
            def blocks(run):
                for n, (job_layer, job_half) in enumerate(jobs):
                    if job_half == ATTN:

                        @pl.when(layer == job_layer)
                        def _(n=n):
                            run(scatters[4 * n])

            bwd_attn_compute(
                dims, step, lambda: rider.at(index, 1, lambda at: (at // steps) % 2 == 1), vec_s.at[layer], wqkv_s.at[layer], wproj_s.at[layer],
                attn_in, work_scratch, groups[ATTN], blocks,
            )

        @pl.when(index > last - steps)
        def _():
            for g in range(PER_STEP):
                start = pl.multiple_of(base + g * dims.rows, 16)
                image_put(dims, wide, step * PER_STEP + g, stream[pl.ds(start, dims.seq), :])

        rider.at(index, 2)

    sem = DMA(Scatter.semaphores(cube))
    lead = lambda i: (LAYERS - 1 - i // (2 * steps)) * steps
    is_attn = lambda i: (i // steps) % 2
    attn_spec = lambda n: pl.BlockSpec((dims.blk, n), lambda i: (lead(i) + (i % steps) * is_attn(i), 0))
    mlp_spec = lambda n: pl.BlockSpec((dims.blk, n), lambda i: (lead(i) + (i % steps) * (1 - is_attn(i)) + (steps - 1) * is_attn(i), 0))
    whole_shapes = [w.shape for w in whole]
    outs = pl.pallas_call(
        body,
        grid=(last + 1,),
        in_specs=[SM, full(grad.shape)]
        + [ANY] * 5
        + [attn_spec(s.shape[1]) for s in saved_attn]
        + [mlp_spec(s.shape[1]) for s in saved_mlp],
        out_specs=[full(wide_shape(dims))] + [full(groups[h].block) for _, h in jobs],
        out_shape=[SDS(wide_shape(dims), F32)] + [SDS(groups[h].block, F32) for _, h in jobs],
        scratch_shapes=[
            pltpu.VMEM((tot, width), F32),
            pltpu.VMEM((2, tot, width), BF),
            pltpu.VMEM((tot, ff), BF),
            pltpu.VMEM((tot, ff), BF),
            pltpu.VMEM((VECS, ff), F32),
            pltpu.VMEM((VECS, LANES), F32),
            pltpu.VMEM((width, ff), BF),
            pltpu.VMEM((ff, width), BF),
            pltpu.VMEM((dims.blk + KEYS - dims.rows, 3 * width), BF),
            DMA((LAYERS, 5)),
        ]
        + [pltpu.VMEM(w.shape, w.dtype) for w in whole]
        + sum([[pltpu.VMEM(groups[h].buffer, BF), pltpu.VMEM(groups[h].buffer, BF), sem, sem] for _, h in jobs], []),
        compiler_params=params_of(1),
        name="backward",
    )(live, grad, *whole, *saved_attn, *saved_mlp)
    return outs[0], dict(zip(jobs, outs[1:]))


def emit_outputs(dims, groups, hidden, grad, sums, params):
    def body(*refs):
        (hidden_ref, grad_ref), blocks, (out_ref, in_grad_ref), outs = take(refs, 2, 2 * LAYERS, 2, 12)
        (n1g, n1b, wqkv, bqv, wproj, bpj, n2g, n2b, w1, bf1, w2, bf2) = outs
        weights = ([wqkv, wproj], [w1, w2])
        vectors = ((n1g, n1b, bpj, bqv, n2g, n2b, bf2, bf1), ())
        for c in range(hidden_ref.shape[0]):
            lanes = slice(c * LANES, (c + 1) * LANES)
            out_ref[:, lanes] = hidden_ref[c].astype(BF)
            in_grad_ref[:, lanes] = grad_ref[c]
        for layer in range(LAYERS):
            for half in (ATTN, MLP):
                groups[half].emit(layer, blocks[2 * layer + half], weights[half], vectors[half])

    return pl.pallas_call(
        body,
        in_specs=[VM] * (2 + 2 * LAYERS),
        out_specs=[VM] * 14,
        out_shape=[SDS((dims.flat, dims.width), BF), SDS((dims.flat, dims.width), F32)] + [SDS(p.shape, F32) for p in params],
        compiler_params=params_of(),
        name="emit",
    )(hidden, grad, *[sums[layer, half] for layer in range(LAYERS) for half in (ATTN, MLP)])


def per_device(devices, inputs, out_grad, live_counts, *params):
    cube = Cube(devices)
    images, seq, width = inputs.shape
    dims = Dims(images, live_counts.shape[0], seq, width, params[9].shape[1] * devices)
    size = lambda *which: [params[i].shape[1] for i in which]
    groups = [
        Group(cube, [params[2].shape[1:], params[4].shape[1:]], size(0, 1, 5, 3, 6, 7, 11, 9)),
        Group(cube, [params[8].shape[1:], params[10].shape[1:]], []),
    ]
    lay = lambda a: a.transpose(1, 0, 2).reshape(dims.flat, width)
    unlay = lambda a: a.reshape(seq, images, width).transpose(1, 0, 2)
    turn = lambda a: a.transpose(1, 0, 2) if a.ndim == 3 and a.shape[1 if a.shape[0] == LAYERS else 0] % 8 else a
    turned = [turn(p) for p in params]
    hidden, whole, saved_attn, saved_mlp = forward(cube, dims, groups, live_counts, lay(inputs), turned)
    grad, sums = backward(cube, dims, groups, live_counts, lay(out_grad), whole, saved_attn, saved_mlp)
    outputs, in_grad, *grads = emit_outputs(dims, groups, hidden, grad, sums, turned)
    return (unlay(outputs), unlay(in_grad), *[turn(g) for g in grads])


def solution(mesh):
    devices = mesh.shape["fsdp"]
    rows3, flat2, rows2 = P("fsdp", None, None), P(None, "fsdp"), P(None, "fsdp", None)
    param_specs = (flat2, flat2, rows2, flat2, rows2, flat2, flat2, flat2, rows2, flat2, rows2, flat2)
    return jax.shard_map(
        functools.partial(per_device, devices),
        mesh=mesh,
        in_specs=(rows3, rows3, P("fsdp")) + param_specs,
        out_specs=(rows3, rows3) + param_specs,
        check_vma=False,
    )
```

```python
import functools
import math

import jax
import jax.numpy as jnp
from jax import lax
from jax.experimental import pallas as pl
from jax.experimental.pallas import tpu as pltpu
from jax.sharding import PartitionSpec as P

HEAD_DIM = 64
LAYERS = 2
EPS = 1e-06
BF = jnp.bfloat16
F32 = jnp.float32
NN = (((1,), (0,)), ((), ()))
NT = (((1,), (1,)), ((), ()))
TN = (((0,), (0,)), ((), ()))
KEYS = 256
LANES = 128
VMEM_LIMIT = 67_000_000
PER_STEP = 2
MESH_ID = pl.DeviceIdType.MESH
N1G, N1B, BPJ, BQV, N2G, N2B, BF2, BF1 = range(8)
VECS = 8
ATTN, MLP = 0, 1
COLORS = 2


def torus_shape(devices):
    return {16: (4, 2, 2), 64: (4, 4, 4)}.get(devices // 2, (1, 1, devices // 2))


class Cube:
    def __init__(self, devices):
        self.devices = devices
        self.axes = []
        stride = devices
        for extent in torus_shape(devices):
            stride //= extent
            if extent > 1:
                self.axes.append((extent, stride))
        by_axis, self.bits = [], 0
        for extent, _ in self.axes:
            count = extent.bit_length() - 1
            by_axis.append(list(range(self.bits, self.bits + count)))
            self.bits += count
        self.slots = 1 << self.bits
        orders = [by_axis, by_axis[:1] + by_axis[:0:-1]]
        self.orders = [sum(order, []) for order in orders]

    def bits_of(self, device):
        bits = []
        for extent, stride in self.axes:
            pos = (device // stride) % extent
            bits += [pos // 2, (pos + pos // 2) % 2] if extent == 4 else [pos]
        return bits

    def order(self, color, step):
        return self.orders[color][step]

    def flat(self, color, bits, first=0):
        return sum(bits[self.order(color, s)] * (1 << s) for s in range(first, self.bits))

    def place(self, color, device):
        return device % 2, color, self.flat(color, self.bits_of(device))

    def position(self):
        me = lax.axis_index("fsdp")
        partners = []
        for extent, stride in self.axes:
            pos = (me // stride) % extent
            if extent == 4:
                partners += [me + (3 - 2 * pos) * stride, me + (1 - 2 * (pos % 2)) * stride]
            else:
                partners += [me + (1 - 2 * pos) * stride]
        return self.bits_of(me), me % 2, partners, me + 1 - 2 * (me % 2)


def greet(partners):
    barrier = pltpu.get_barrier_semaphore()
    for partner in partners:
        pl.semaphore_signal(barrier, inc=1, device_id=(partner,), device_id_type=MESH_ID)
    pl.semaphore_wait(barrier, len(partners))


class Group:
    def __init__(self, cube, shapes, sizes):
        self.cube, self.sizes = cube, sizes
        self.rows = min(rows for rows, _ in shapes)
        units = [
            (a, q, c) for a, (rows, lanes) in enumerate(shapes) for c in range(lanes // LANES) for q in range(rows // self.rows)
        ]
        share = -(-len(units) // COLORS)
        self.units = [(i // share, i % share * self.rows, *unit) for i, unit in enumerate(units)]
        self.vec_row = share * self.rows
        self.vec_row += self.vec_row % 2
        self.height = -(-(self.vec_row + (VECS if sizes else 0)) // 16) * 16
        self.pack = 16 // math.gcd(self.rows, 16)

    @property
    def block(self):
        return (COLORS, self.height, LANES)

    @property
    def buffer(self):
        return (2, COLORS, self.cube.slots, self.height, LANES)

    def runs(self):
        return [(i, i + 1 if i % 4 == 3 else i + 3, self.sizes[i]) for i in (0, 3, 4, 7)]

    def pack_own(self, layer, weights, vectors, temp, store):
        for color, row, a, q, c in self.units:
            lanes = slice(c * LANES, (c + 1) * LANES)
            span = slice(q * self.rows, (q + 1) * self.rows)
            at = (span, layer, lanes) if weights[a].shape[1] == LAYERS else (layer, span, lanes)
            store(color, row, row + self.rows, weights[a][at])
        if self.sizes:
            for i, vector in enumerate(vectors):
                temp[i : i + 1, : vector.shape[1]] = vector[layer : layer + 1, :].astype(F32)
            store(0, self.vec_row, self.vec_row + VECS, temp[...].astype(BF))

    def place(self, color, first, i):
        return self.cube.place(color, first + i)

    def spread(self, buf, targets, vec):
        merged = self.rows % 4 == 0

        def natural(g, _):
            first = g * self.pack
            for a, target in enumerate(targets):
                rows = target.shape[0] // self.cube.devices
                pieces = rows // self.rows
                count = self.pack
                by_lane = {}
                for color, row, b, q, c in self.units:
                    if b == a:
                        by_lane.setdefault(c, {})[q] = (color, row)
                for c, places in by_lane.items():
                    parts = []
                    for i in range(count):
                        for q in range(pieces):
                            color, row = places[q]
                            part = buf[self.place(color, first, i) + (slice(row, row + self.rows), slice(None))]
                            parts.append(part if merged else part.astype(F32))
                    value = jnp.concatenate(parts, axis=0).astype(target.dtype)
                    height = count * rows
                    target[pl.ds(pl.multiple_of(g * height, 16), height), c * LANES : (c + 1) * LANES] = value
            return 0

        lax.fori_loop(0, self.cube.devices // self.pack, natural, 0)
        for d in range(self.cube.devices if self.sizes else 0):
            value = buf[self.place(0, d, 0) + (slice(self.vec_row, self.vec_row + VECS), slice(None))].astype(F32)
            for lo, hi, size in self.runs():
                vec[lo:hi, d * size : (d + 1) * size] = value[lo:hi, :size]

    def split(self, sources, vec, temp, buf):
        merged = self.rows % 4 == 0

        def natural(g, _):
            first = g * self.pack
            for color, row, a, q, c in self.units:
                rows = sources[a].shape[0] // self.cube.devices
                height = self.pack * rows
                value = sources[a][pl.ds(pl.multiple_of(g * height, 16), height), c * LANES : (c + 1) * LANES]
                if not merged:
                    value = value.astype(F32)
                for i in range(self.pack):
                    lo = i * rows + q * self.rows
                    buf[self.place(color, first, i) + (slice(row, row + self.rows), slice(None))] = value[lo : lo + self.rows].astype(BF)
            return 0

        lax.fori_loop(0, self.cube.devices // self.pack, natural, 0)
        for d in range(self.cube.devices if self.sizes else 0):
            for lo, hi, size in self.runs():
                temp[lo:hi, :size] = vec[lo:hi, d * size : (d + 1) * size]
            buf[self.place(0, d, 0) + (slice(self.vec_row, self.vec_row + VECS), slice(None))] = temp[...].astype(BF)

    def emit(self, layer, block, weights, vectors):
        for color, row, a, q, c in self.units:
            lanes = slice(c * LANES, (c + 1) * LANES)
            span = slice(q * self.rows, (q + 1) * self.rows)
            at = (span, layer, lanes) if weights[a].shape[1] == LAYERS else (layer, span, lanes)
            weights[a][at] = block[color, row : row + self.rows, :]
        for i, vector in enumerate(vectors):
            vector[layer : layer + 1, :] = block[0, self.vec_row + i : self.vec_row + i + 1, : vector.shape[1]]


class Gather:
    def __init__(self, group, position, source, buf, send, recv):
        self.cube, self.group = group.cube, group
        self.mine, self.core, self.partners, self.other = position
        self.source, self.buf, self.send, self.recv = source, buf, send, recv
        self.ticks = self.cube.bits + 2

    @staticmethod
    def semaphores(cube):
        return (COLORS * cube.bits + 1,)

    def copy(self, color, step):
        cube = self.cube
        if step == cube.bits:
            key, partner = COLORS * cube.bits, self.other
            src = dst = self.buf.at[self.core]
        else:
            key, partner = color * cube.bits + step, self.partners[cube.order(color, step)]
            dst = self.buf.at[self.core, color, pl.ds(cube.flat(color, self.mine, step), 1 << step)]
            src = self.source.at[pl.ds(color, 1)] if step == 0 else dst
        return pltpu.make_async_remote_copy(
            src_ref=src,
            dst_ref=dst,
            send_sem=self.send.at[key],
            recv_sem=self.recv.at[key],
            device_id=(partner,),
            device_id_type=MESH_ID,
        )

    def local(self, sem):
        return [
            pltpu.make_async_copy(
                self.source.at[pl.ds(c, 1)], self.buf.at[self.core, c, pl.ds(self.cube.flat(c, self.mine), 1)], sem.at[c]
            )
            for c in range(COLORS)
        ]

    def tick(self, t):
        bits = self.cube.bits
        for color in range(COLORS):
            if 0 < t <= bits:
                self.copy(color, t - 1).wait_recv()
            if t < bits:
                self.copy(color, t).start()
        if t == bits:
            self.copy(0, bits).start()
        if t > bits:
            self.copy(0, bits).wait()
            for color in range(COLORS):
                for step in range(bits):
                    self.copy(color, step).wait_send()


class Scatter:
    def __init__(self, group, position, blocks, inbox, out, send, recv):
        self.cube = group.cube
        self.mine, self.core, self.partners, self.other = position
        self.blocks, self.inbox, self.out, self.send, self.recv = blocks, inbox, out, send, recv
        self.ticks = self.cube.bits + 2

    @staticmethod
    def semaphores(cube):
        return (COLORS * cube.bits + 1,)

    def copy(self, color, step):
        cube = self.cube
        if step == cube.bits:
            key, partner = COLORS * cube.bits, self.other
            src, dst = self.blocks.at[1 - self.core], self.inbox.at[0]
        else:
            key, partner = color * cube.bits + step, self.partners[cube.order(color, step)]
            size = 1 << step
            start = cube.flat(color, self.mine, step) + (1 - 2 * self.mine[cube.order(color, step)]) * size
            src = self.blocks.at[self.core, color, pl.ds(start, size)]
            dst = self.inbox.at[1, color, pl.ds(size, size)]
        return pltpu.make_async_remote_copy(
            src_ref=src,
            dst_ref=dst,
            send_sem=self.send.at[key],
            recv_sem=self.recv.at[key],
            device_id=(partner,),
            device_id_type=MESH_ID,
        )

    def absorb(self, color, step):
        cube = self.cube
        if step == cube.bits:
            start, size, base, box = 0, cube.slots, 0, 0
        else:
            start, size, base, box = cube.flat(color, self.mine, step), 1 << step, 1 << step, 1
        if step == 0:
            self.out[color] = self.blocks[self.core, color, start].astype(F32) + self.inbox[box, color, base].astype(F32)
            return

        def body(j, _):
            at = (self.core, color, start + j)
            self.blocks[at] = self.blocks[at] + self.inbox[box, color, base + j]
            return 0

        lax.fori_loop(0, size, body, 0)

    def tick(self, t):
        bits = self.cube.bits
        if t == 0:
            self.copy(0, bits).start()
            return
        if t == 1:
            self.copy(0, bits).wait_recv()
        for color in range(COLORS):
            if t > 1:
                self.copy(color, bits + 1 - t).wait_recv()
            self.absorb(color, bits + 1 - t)
            if t <= bits:
                self.copy(color, bits - t).start()
        if t == bits + 1:
            self.copy(0, bits).wait_send()
            for color in range(COLORS):
                for step in range(bits):
                    self.copy(color, step).wait_send()


class Rider:
    def __init__(self):
        self.due = {}

    def add(self, step, point, run):
        self.due.setdefault((step, point), []).append(run)

    def at(self, index, point, where=lambda step: True):
        for (step, slot), runs in sorted(self.due.items(), key=lambda item: item[0]):
            if slot == point and where(step):

                @pl.when(index == step)
                def _(runs=runs):
                    for run in runs:
                        run()


def mm(left, right, dims):
    return lax.dot_general(left, right, dims, preferred_element_type=F32)


def norm_stats(hidden):
    centered = hidden - jnp.mean(hidden, axis=-1, keepdims=True)
    inv_std = lax.rsqrt(jnp.mean(centered * centered, axis=-1, keepdims=True) + EPS)
    return centered * inv_std, inv_std


def norm_back(grad_in, normed, inv_std, gain):
    dnorm = grad_in * gain
    return inv_std * (
        dnorm
        - jnp.mean(dnorm, axis=-1, keepdims=True)
        - normed * jnp.mean(dnorm * normed, axis=-1, keepdims=True)
    )


def half_masks():
    lane = lax.broadcasted_iota(jnp.int32, (1, LANES), 1)
    low = (lane < HEAD_DIM).astype(F32).astype(BF)
    return low, 1 - low


class Dims:
    def __init__(self, images, counts, seq, width, ff):
        self.images, self.slots, self.seq, self.width, self.ff = images, images // counts, seq, width, ff
        self.rows = -(-seq // 16) * 16
        self.steps = images // PER_STEP
        self.blk = PER_STEP * self.rows
        self.tot = images * self.rows
        self.flat = images * seq


def vrow(vec_ref, row, width, start=0):
    return vec_ref[row : row + 1, start : start + width]


def image_rows(dims, image):
    return pl.ds(image, dims.seq, stride=dims.images)


def wide_shape(dims):
    return (dims.width // LANES, dims.flat, LANES)


def wide_load(wide, ref):
    for c in range(wide.shape[0]):
        wide[c] = ref[:, c * LANES : (c + 1) * LANES].astype(F32)


def image_get(dims, wide, image):
    return jnp.concatenate([wide[c, image_rows(dims, image), :] for c in range(wide.shape[0])], axis=1)


def image_put(dims, wide, image, value):
    for c in range(wide.shape[0]):
        wide[c, image_rows(dims, image), :] = value[:, c * LANES : (c + 1) * LANES]


def alive(counts, dims, group, slot):
    return jnp.clip(counts[group] - slot, 0, 1).astype(F32)


def fwd_attn_compute(dims, base, vec_ref, wqkv_ref, wproj_ref, outs, scratch):
    n1_ref, inv_ref, qkv_out, e_ref, il_ref, ctx_ref = outs
    stream, qkv_ref = scratch
    width, rows, seq, total = dims.width, dims.rows, dims.seq, dims.blk
    span = pl.ds(base, total)
    h = stream[span, :]
    n1, inv1 = norm_stats(h)
    n1_ref[...] = n1.astype(BF)
    inv_ref[...] = jnp.broadcast_to(inv1, inv_ref.shape)
    attn_in = (n1 * vrow(vec_ref, N1G, width) + vrow(vec_ref, N1B, width)).astype(BF)
    q = (mm(attn_in, wqkv_ref[:, :width], NN) + vrow(vec_ref, BQV, width)).astype(BF) * BF(HEAD_DIM ** -0.5)
    k = mm(attn_in, wqkv_ref[:, width : 2 * width], NN).astype(BF)
    v = (mm(attn_in, wqkv_ref[:, 2 * width :], NN) + vrow(vec_ref, BQV, width, width)).astype(BF)
    for i, part in enumerate((q, k, v)):
        qkv_ref[0:total, i * width : (i + 1) * width] = part
        qkv_out[:, i * width : (i + 1) * width] = part
    low, high = half_masks()
    lane = lax.broadcasted_iota(jnp.int32, (1, KEYS), 1)
    key_mask = jnp.where(lane < seq, 0.0, -1e30).astype(F32)
    lane_low = lax.broadcasted_iota(jnp.int32, (1, LANES), 1) < HEAD_DIM
    ones = jnp.ones((KEYS, LANES), BF)
    for g in range(PER_STEP):
        r0 = g * rows
        for pair in range(width // LANES):
            c0 = pair * LANES
            qp = qkv_ref[r0 : r0 + rows, c0 : c0 + LANES]
            kp = qkv_ref[r0 : r0 + KEYS, width + c0 : width + c0 + LANES]
            vp = qkv_ref[r0 : r0 + KEYS, 2 * width + c0 : 2 * width + c0 + LANES]
            vo = jnp.concatenate([vp, ones], axis=1)
            parts = []
            for half, mask in enumerate((low, high)):
                s = mm(qp * mask, kp, NT) + key_mask
                e = jnp.exp(s - jnp.max(s, axis=-1, keepdims=True)).astype(BF)
                j = 2 * pair + half
                e_ref[r0 : r0 + rows, j * KEYS : (j + 1) * KEYS] = e
                r = mm(e, vo, NN)
                recip = 1.0 / r[:, LANES:]
                parts.append((r[:, :LANES] * recip, recip))
            ctx_ref[r0 : r0 + rows, c0 : c0 + LANES] = jnp.where(lane_low, parts[0][0], parts[1][0]).astype(BF)
            il_ref[r0 : r0 + rows, c0 : c0 + LANES] = jnp.where(lane_low, parts[0][1], parts[1][1])
    stream[span, :] = h + mm(ctx_ref[...], wproj_ref[...], NN) + vrow(vec_ref, BPJ, width)


def fwd_mlp_compute(dims, base, vec_ref, w1_ref, w2_ref, outs, stream):
    n2_ref, inv_ref, act_ref, slope_ref = outs
    width, span = dims.width, pl.ds(base, dims.blk)
    mid = stream[span, :]
    n2, inv2 = norm_stats(mid)
    n2_ref[...] = n2.astype(BF)
    inv_ref[...] = jnp.broadcast_to(inv2, inv_ref.shape)
    mlp_in = (n2 * vrow(vec_ref, N2G, width) + vrow(vec_ref, N2B, width)).astype(BF)
    chunk = 256
    for c in range(0, dims.ff, chunk):
        pre = mm(mlp_in, w1_ref[:, c : c + chunk], NN) + vrow(vec_ref, BF1, chunk, c)
        cdf = 0.5 + 0.5 * lax.erf(pre * 0.7071067811865476)
        act_ref[:, c : c + chunk] = (pre * cdf).astype(BF)
        slope_ref[:, c : c + chunk] = (cdf + pre * jnp.exp(-0.5 * pre * pre) * 0.3989422804014327).astype(BF)
    stream[span, :] = mid + mm(act_ref[...], w2_ref[...], NN) + vrow(vec_ref, BF2, width)


def bwd_mlp_compute(dims, step, poll, vec_ref, w1_ref, w2_ref, saved, scratch, group, blocks):
    n2_ref, inv_ref, act_ref, slope_ref = saved
    stream, thin, act_all, dpre_all, vecs_ref, temp, dw_ref, dw2_ref, _ = scratch
    width, total = dims.width, dims.blk
    gb_all, mlp_all = thin.at[0], thin.at[1]
    span = pl.ds(pl.multiple_of(step * total, 16), total)

    @pl.when(step == 0)
    def _():
        vecs_ref[...] = jnp.zeros_like(vecs_ref)

    gh = stream[span, :]
    gb = gh.astype(BF)
    gb_all[span, :] = gb
    act_all[span, :] = act_ref[...]
    vecs_ref[BF2 : BF2 + 1, :width] += jnp.sum(gh, axis=0, keepdims=True)
    chunk = 256
    for c in range(0, dims.ff, chunk):
        dpre = mm(gb, w2_ref[c : c + chunk, :], NT) * slope_ref[:, c : c + chunk].astype(F32)
        vecs_ref[BF1 : BF1 + 1, c : c + chunk] += jnp.sum(dpre, axis=0, keepdims=True)
        dpre_all[span, c : c + chunk] = dpre.astype(BF)
    poll()
    dmlp = mm(dpre_all[span, :], w1_ref[...], NT)
    n2 = n2_ref[...].astype(F32)
    mlp_all[span, :] = (n2 * vrow(vec_ref, N2G, width) + vrow(vec_ref, N2B, width)).astype(BF)
    vecs_ref[N2G : N2G + 1, :width] += jnp.sum(dmlp * n2, axis=0, keepdims=True)
    vecs_ref[N2B : N2B + 1, :width] += jnp.sum(dmlp, axis=0, keepdims=True)
    gm = gh + norm_back(dmlp, n2, inv_ref[:, 0:1], vrow(vec_ref, N2G, width))
    vecs_ref[BPJ : BPJ + 1, :width] += jnp.sum(gm, axis=0, keepdims=True)
    stream[span, :] = gm

    @pl.when(step == dims.steps - 1)
    def _():
        for c in range(0, dims.ff, 512):
            dw_ref[:, c : c + 512] = mm(mlp_all[...], dpre_all[:, c : c + 512], TN).astype(BF)
            dw2_ref[c : c + 512, :] = mm(act_all[:, c : c + 512], gb_all[...], TN).astype(BF)
        blocks(lambda buf: group.split([dw_ref, dw2_ref], None, temp, buf))


def bwd_attn_compute(dims, step, poll, vec_ref, wqkv_ref, wproj_ref, saved, scratch, group, blocks):
    n1_ref, inv_ref, qkv_in, e_ref, il_ref, ctx_ref = saved
    stream, thin, several, dqkv_all, vecs_ref, temp, dw_ref, _, qkv_ref = scratch
    width, rows, total = dims.width, dims.rows, dims.blk
    gmb_all, ctx_all = thin.at[0], thin.at[1]
    base = pl.multiple_of(step * total, 16)
    span = pl.ds(base, total)
    qkv_ref[0:total, :] = qkv_in[...]
    gm = stream[span, :]
    gmb = gm.astype(BF)
    gmb_all[span, :] = gmb
    ctx_all[span, :] = ctx_ref[...]
    dctx = mm(gmb, wproj_ref[...], NT).astype(BF).astype(F32) * il_ref[...]
    dos_all = dctx.astype(BF)
    doo = dos_all.astype(F32) * ctx_ref[...].astype(F32)
    doo_high = doo.astype(BF)
    doo_low = doo - doo_high.astype(F32)
    lane_low = lax.broadcasted_iota(jnp.int32, (1, LANES), 1) < HEAD_DIM
    low, high = half_masks()
    minus = jnp.full((KEYS, LANES), -1.0, BF)
    for g in range(PER_STEP):
        r0 = g * rows
        rr = pl.ds(pl.multiple_of(base + r0, 16), rows)
        for pair in range(width // LANES):
            c0 = pair * LANES
            qp = qkv_ref[r0 : r0 + rows, c0 : c0 + LANES]
            kp = qkv_ref[r0 : r0 + KEYS, width + c0 : width + c0 + LANES]
            vp = qkv_ref[r0 : r0 + KEYS, 2 * width + c0 : 2 * width + c0 + LANES]
            vm = jnp.concatenate([vp, minus], axis=1)
            dos = dos_all[r0 : r0 + rows, c0 : c0 + LANES]
            upper = doo_high[r0 : r0 + rows, c0 : c0 + LANES].astype(F32)
            lower = pltpu.roll(doo_low[r0 : r0 + rows, c0 : c0 + LANES], HEAD_DIM, 1)
            dots = [jnp.where(lane_low, a, b).astype(BF) for a, b in ((upper, lower), (lower, upper))]
            dq = dk = dv = None
            for half, mask in enumerate((low, high)):
                j = 2 * pair + half
                e = e_ref[r0 : r0 + rows, j * KEYS : (j + 1) * KEYS]
                dd = mm(jnp.concatenate([dos * mask, dots[half]], axis=1), vm, NT)
                ds = (e.astype(F32) * dd).astype(BF)
                dv_h = mm(e, dos * mask, TN)
                dk_h = mm(ds, qp * mask, TN)
                dq_h = mm(ds, kp * mask, NN)
                dq = dq_h if dq is None else dq + dq_h
                dk = dk_h if dk is None else dk + dk_h
                dv = dv_h if dv is None else dv + dv_h
            dq = dq * (HEAD_DIM ** -0.5)
            dv = dv[:rows]
            vecs_ref[BQV : BQV + 1, c0 : c0 + LANES] += jnp.sum(dq, axis=0, keepdims=True)
            vecs_ref[BQV : BQV + 1, width + c0 : width + c0 + LANES] += jnp.sum(dv, axis=0, keepdims=True)
            dqkv_all[rr, c0 : c0 + LANES] = dq.astype(BF)
            dqkv_all[rr, width + c0 : width + c0 + LANES] = dk[:rows].astype(BF)
            dqkv_all[rr, 2 * width + c0 : 2 * width + c0 + LANES] = dv.astype(BF)
    poll()
    dai = mm(dqkv_all[span, : 3 * width], wqkv_ref[...], NT)
    n1 = n1_ref[...].astype(F32)
    several[span, :width] = (n1 * vrow(vec_ref, N1G, width) + vrow(vec_ref, N1B, width)).astype(BF)
    vecs_ref[N1G : N1G + 1, :width] += jnp.sum(dai * n1, axis=0, keepdims=True)
    vecs_ref[N1B : N1B + 1, :width] += jnp.sum(dai, axis=0, keepdims=True)
    stream[span, :] = gm + norm_back(dai, n1, inv_ref[:, 0:1], vrow(vec_ref, N1G, width))

    @pl.when(step == dims.steps - 1)
    def _():
        for c in range(0, 3 * width, width):
            dw_ref[:, c : c + width] = mm(several[:, :width], dqkv_all[:, c : c + width], TN).astype(BF)
        dw_ref[:, 3 * width : 4 * width] = mm(ctx_all[...], gmb_all[...], TN).astype(BF)
        blocks(lambda buf: group.split([dw_ref.at[:, : 3 * width], dw_ref.at[:, 3 * width : 4 * width]], vecs_ref, temp, buf))


ANY = pl.BlockSpec(memory_space=pl.ANY)
VM = pl.BlockSpec(memory_space=pltpu.VMEM)
SM = pl.BlockSpec(memory_space=pltpu.SMEM)
SDS = jax.ShapeDtypeStruct
DMA = pltpu.SemaphoreType.DMA


def full(shape):
    return pl.BlockSpec(shape, lambda i: (0,) * len(shape), pipeline_mode=pl.Buffered(1))


def take(refs, *counts):
    refs, parts = list(refs), []
    for count in counts:
        parts.append(refs[:count])
        refs = refs[count:]
    assert not refs
    return parts


def params_of(collective=None):
    extra = {} if collective is None else {"collective_id": collective, "has_side_effects": True}
    return pltpu.CompilerParams(vmem_limit_bytes=VMEM_LIMIT, **extra)


def weight_shapes(dims):
    return [(dims.width, 3 * dims.width), (dims.width, dims.width), (dims.width, dims.ff), (dims.ff, dims.width)]


def forward(cube, dims, groups, live, x, params):
    steps, width, ff, tot = dims.steps, dims.width, dims.ff, dims.tot
    shapes = weight_shapes(dims)
    jobs = [(layer, half) for layer in range(LAYERS) for half in (ATTN, MLP)]
    heads = (width // HEAD_DIM) * KEYS
    saved_attn = [(width, BF), (LANES, F32), (3 * width, BF), (heads, BF), (width, F32), (width, BF)]
    saved_mlp = [(width, BF), (LANES, F32), (ff, BF), (ff, BF)]
    last = 2 * LAYERS * steps - 1

    def body(*refs):
        (live_ref, x_ref), args, (wide,), whole, attn_outs, mlp_outs, scratch, gathers = take(
            refs, 2, 12, 1, 5, len(saved_attn), len(saved_mlp), 10, 4 * len(jobs)
        )
        (n1g, n1b, wqkv, bqv, wproj, bpj, n2g, n2b, w1, bf1, w2, bf2) = args
        temp, local_sem, out_sem, stream, qkv_ref, *kept = scratch
        vec_s, wqkv_s, wproj_s, w1_s, w2_s = kept
        index = pl.program_id(0)
        layer, half, step = index // (2 * steps), (index // steps) % 2, index % steps
        base = pl.multiple_of(step * dims.blk, 16)
        position = cube.position()
        weights = ([wqkv, wproj], [w1, w2])
        vectors = ((n1g, n1b, bpj, bqv, n2g, n2b, bf2, bf1), ())
        works = []
        for n, (job_layer, job_half) in enumerate(jobs):
            own, buf, send, recv = gathers[4 * n : 4 * n + 4]
            works.append(Gather(groups[job_half], position, own, buf, send, recv))
        ticks = works[0].ticks

        def pack(n):
            job_layer, job_half = jobs[n]
            own = gathers[4 * n]

            def store(color, lo, hi, value):
                own[color, lo:hi, :] = value

            own[...] = jnp.zeros_like(own)
            groups[job_half].pack_own(job_layer, weights[job_half], vectors[job_half], temp, store)

        begins = [0, 2] + [ticks - 1 + 2 * n for n in range(len(jobs) - 2)]

        def tick(n, t):
            if t == 0:
                for copy in works[n].local(local_sem.at[n]):
                    copy.start()
            if t == 1:
                for copy in works[n].local(local_sem.at[n]):
                    copy.wait()
            works[n].tick(t)

        def saves(n):
            job_layer, job_half = jobs[n]
            which = (1, 2, 0) if job_half == ATTN else (3, 4)
            return [
                pltpu.make_async_copy(kept[k].at[job_layer], whole[k].at[job_layer], out_sem.at[job_layer, k]) for k in which
            ]

        def finish(n):
            job_layer, job_half = jobs[n]
            targets = [wqkv_s, wproj_s] if job_half == ATTN else [w1_s, w2_s]
            if job_half == ATTN:
                vec_s[job_layer] = jnp.zeros(vec_s.shape[1:], F32)
            groups[job_half].spread(gathers[4 * n + 1], [t.at[job_layer] for t in targets], vec_s.at[job_layer])
            for copy in saves(n):
                copy.start()

        def begin():
            temp[...] = jnp.zeros_like(temp)
            pack(0)
            greet(position[2] + [position[3]])
            for t in range(ticks):
                for n in range(len(jobs)):
                    if 0 <= t - begins[n] < ticks:
                        tick(n, t - begins[n])
                if t + 1 < len(jobs):
                    pack(t + 1)
                if t == 2:
                    qkv_ref[dims.blk :, :] = jnp.zeros_like(qkv_ref[dims.blk :, :])
                    stream[...] = jnp.zeros_like(stream)
                    wide_load(wide, x_ref)
                    for image in range(dims.images):
                        stream[image * dims.rows : image * dims.rows + dims.seq, :] = image_get(dims, wide, image)
            finish(0)

        rider = Rider()
        rider.add(0, 0, begin)
        timed = [(), (0, 0, 0, 0, 3, 4), (0, 1, 2, 3, 5, 7), (2, 4, 6, 8, 11, 12)]
        for late in range(ticks, begins[-1] + ticks):
            at = late - ticks + 1
            at += at // steps
            for n in range(1, len(jobs)):
                if 0 <= late - begins[n] < ticks:
                    t = late - begins[n]
                    poll = timed[n][t] if ticks == 6 and steps == 4 and n < len(timed) else at
                    rider.add(min(poll, n * steps), 0, lambda n=n, t=t: tick(n, t))
        for n in range(1, len(jobs)):
            rider.add(n * steps, 0, lambda n=n: finish(n))
        rider.at(index, 0)

        @pl.when(half == ATTN)
        def _():
            fwd_attn_compute(
                dims, base, vec_s.at[layer], wqkv_s.at[layer], wproj_s.at[layer], attn_outs, (stream, qkv_ref)
            )

        @pl.when(half == MLP)
        def _():
            fwd_mlp_compute(dims, base, vec_s.at[layer], w1_s.at[layer], w2_s.at[layer], mlp_outs, stream)

        @pl.when(index > last - steps)
        def _():
            for g in range(PER_STEP):
                start = pl.multiple_of(base + g * dims.rows, 16)
                group, slot = step * (PER_STEP // dims.slots) + g // dims.slots, g % dims.slots
                image_put(dims, wide, step * PER_STEP + g, stream[pl.ds(start, dims.seq), :] * alive(live_ref, dims, group, slot))

        @pl.when(index == last)
        def _():
            for n in range(len(jobs)):
                for copy in saves(n):
                    copy.wait()

    sem = DMA(Gather.semaphores(cube))
    lead = lambda i: (i // (2 * steps)) * steps
    half_of = lambda i: (i // steps) % 2
    attn_spec = lambda n: pl.BlockSpec((dims.blk, n), lambda i: (lead(i) + (i % steps) * (1 - half_of(i)) + (steps - 1) * half_of(i), 0))
    mlp_spec = lambda n: pl.BlockSpec((dims.blk, n), lambda i: (lead(i) + (i % steps) * half_of(i), 0))
    whole_shapes = [(LAYERS, VECS, ff)] + [(LAYERS,) + s for s in shapes]
    whole_types = [F32, BF, BF, BF, BF]
    outs = pl.pallas_call(
        body,
        grid=(last + 1,),
        in_specs=[SM, full(x.shape)] + [full(p.shape) for p in params],
        out_specs=[full(wide_shape(dims))]
        + [ANY] * 5
        + [attn_spec(n) for n, _ in saved_attn]
        + [mlp_spec(n) for n, _ in saved_mlp],
        out_shape=[SDS(wide_shape(dims), F32)]
        + [SDS(s, t) for s, t in zip(whole_shapes, whole_types)]
        + [SDS((LAYERS * tot, n), t) for n, t in saved_attn + saved_mlp],
        scratch_shapes=[
            pltpu.VMEM((VECS, LANES), F32),
            DMA((len(jobs), COLORS)),
            DMA((LAYERS, 5)),
            pltpu.VMEM((tot, width), F32),
            pltpu.VMEM((dims.blk + KEYS - dims.rows, 3 * width), BF),
        ]
        + [pltpu.VMEM(s, t) for s, t in zip(whole_shapes, whole_types)]
        + sum([[pltpu.VMEM(groups[h].block, BF), pltpu.VMEM(groups[h].buffer, BF), sem, sem] for _, h in jobs], []),
        compiler_params=params_of(0),
        name="forward",
    )(live, x, *params)
    return outs[0], outs[1:6], outs[6:12], outs[12:16]


def spread_ticks(ticks, polls):
    return polls if ticks == len(polls) else [polls[t * len(polls) // ticks] for t in range(ticks)]


def backward(cube, dims, groups, live, grad, whole, saved_attn, saved_mlp):
    steps, width, ff, tot = dims.steps, dims.width, dims.ff, dims.tot
    jobs = [(layer, half) for layer in reversed(range(LAYERS)) for half in (MLP, ATTN)]
    last = len(jobs) * steps - 1

    def body(*refs):
        (live_ref, og_ref), whole_in, attn_in, mlp_in, (wide,), sums, scratch, kept, scatters = take(
            refs, 2, 5, 6, 4, 1, len(jobs), 10, 5, 4 * len(jobs)
        )
        *work_scratch, load_sem = scratch
        stream, qkv_ref = work_scratch[0], work_scratch[8]
        vec_s, wqkv_s, wproj_s, w1_s, w2_s = kept
        index = pl.program_id(0)
        layer, half, step = LAYERS - 1 - index // (2 * steps), 1 - (index // steps) % 2, index % steps
        base = pl.multiple_of(step * dims.blk, 16)
        position = cube.position()
        works = []
        for n, (job_layer, job_half) in enumerate(jobs):
            blocks, inbox, send, recv = scatters[4 * n : 4 * n + 4]
            works.append(Scatter(groups[job_half], position, blocks, inbox, sums[n], send, recv))
        ticks = works[0].ticks

        def loads(n):
            job_layer, job_half = jobs[n]
            which = (1, 2) if job_half == ATTN else (0, 3, 4)
            return [
                pltpu.make_async_copy(whole_in[k].at[job_layer], kept[k].at[job_layer], load_sem.at[job_layer, k]) for k in which
            ]

        def begin():
            for n in range(len(jobs)):
                for copy in loads(n):
                    copy.start()
            qkv_ref[dims.blk :, :] = jnp.zeros_like(qkv_ref[dims.blk :, :])
            stream[...] = jnp.zeros_like(stream)
            wide_load(wide, og_ref)
            for image in range(dims.images):
                stream[image * dims.rows : image * dims.rows + dims.seq, :] = image_get(dims, wide, image) * alive(
                    live_ref, dims, image // dims.slots, image % dims.slots
                )
            greet(position[2] + [position[3]])

        def ready(n):
            for copy in loads(n):
                copy.wait()

        rider = Rider()
        rider.add(0, 0, begin)
        for n in range(len(jobs)):
            rider.add(n * steps, 0, lambda n=n: ready(n))
        end = (last, 2)
        for n, (job_layer, job_half) in enumerate(jobs):
            first = (n + 1) * steps
            if job_half == MLP:
                polls = [(first, 0), (first + 1, 0), (first + 2, 1), (first + 3, 1), (first + 4, 0), (first + 5, 0)]
            else:
                polls = [(first, 0), (first + 1, 0), (first + 2, 1), (first + 3, 1), (first + 4, 0), (first + 5, 0)]
            for t, (at, point) in enumerate(spread_ticks(ticks, polls)):
                if at <= last:
                    rider.add(at, point, lambda n=n, t=t: works[n].tick(t))
                else:
                    rider.add(*end, lambda n=n, t=t: works[n].tick(t))
        left = rider.due.pop(end)
        count = len(left) - ticks
        order = []
        for t in range(ticks):
            order.append(left[count + t])
            order += left[t : t + 1] if t < count else []
        rider.due[end] = order
        rider.at(index, 0)

        @pl.when(half == MLP)
        def _():
            def blocks(run):
                for n, (job_layer, job_half) in enumerate(jobs):
                    if job_half == MLP:

                        @pl.when(layer == job_layer)
                        def _(n=n):
                            run(scatters[4 * n])

            bwd_mlp_compute(
                dims, step, lambda: rider.at(index, 1, lambda at: (at // steps) % 2 == 0), vec_s.at[layer], w1_s.at[layer], w2_s.at[layer],
                mlp_in, work_scratch, groups[MLP], blocks,
            )

        @pl.when(half == ATTN)
        def _():
            def blocks(run):
                for n, (job_layer, job_half) in enumerate(jobs):
                    if job_half == ATTN:

                        @pl.when(layer == job_layer)
                        def _(n=n):
                            run(scatters[4 * n])

            bwd_attn_compute(
                dims, step, lambda: rider.at(index, 1, lambda at: (at // steps) % 2 == 1), vec_s.at[layer], wqkv_s.at[layer], wproj_s.at[layer],
                attn_in, work_scratch, groups[ATTN], blocks,
            )

        @pl.when(index > last - steps)
        def _():
            for g in range(PER_STEP):
                start = pl.multiple_of(base + g * dims.rows, 16)
                image_put(dims, wide, step * PER_STEP + g, stream[pl.ds(start, dims.seq), :])

        rider.at(index, 2)

    sem = DMA(Scatter.semaphores(cube))
    lead = lambda i: (LAYERS - 1 - i // (2 * steps)) * steps
    is_attn = lambda i: (i // steps) % 2
    attn_spec = lambda n: pl.BlockSpec((dims.blk, n), lambda i: (lead(i) + (i % steps) * is_attn(i), 0))
    mlp_spec = lambda n: pl.BlockSpec((dims.blk, n), lambda i: (lead(i) + (i % steps) * (1 - is_attn(i)) + (steps - 1) * is_attn(i), 0))
    whole_shapes = [w.shape for w in whole]
    outs = pl.pallas_call(
        body,
        grid=(last + 1,),
        in_specs=[SM, full(grad.shape)]
        + [ANY] * 5
        + [attn_spec(s.shape[1]) for s in saved_attn]
        + [mlp_spec(s.shape[1]) for s in saved_mlp],
        out_specs=[full(wide_shape(dims))] + [full(groups[h].block) for _, h in jobs],
        out_shape=[SDS(wide_shape(dims), F32)] + [SDS(groups[h].block, F32) for _, h in jobs],
        scratch_shapes=[
            pltpu.VMEM((tot, width), F32),
            pltpu.VMEM((2, tot, width), BF),
            pltpu.VMEM((tot, ff), BF),
            pltpu.VMEM((tot, ff), BF),
            pltpu.VMEM((VECS, ff), F32),
            pltpu.VMEM((VECS, LANES), F32),
            pltpu.VMEM((width, ff), BF),
            pltpu.VMEM((ff, width), BF),
            pltpu.VMEM((dims.blk + KEYS - dims.rows, 3 * width), BF),
            DMA((LAYERS, 5)),
        ]
        + [pltpu.VMEM(w.shape, w.dtype) for w in whole]
        + sum([[pltpu.VMEM(groups[h].buffer, BF), pltpu.VMEM(groups[h].buffer, BF), sem, sem] for _, h in jobs], []),
        compiler_params=params_of(1),
        name="backward",
    )(live, grad, *whole, *saved_attn, *saved_mlp)
    return outs[0], dict(zip(jobs, outs[1:]))


def emit_outputs(dims, groups, hidden, grad, sums, params):
    def body(*refs):
        (hidden_ref, grad_ref), blocks, (out_ref, in_grad_ref), outs = take(refs, 2, 2 * LAYERS, 2, 12)
        (n1g, n1b, wqkv, bqv, wproj, bpj, n2g, n2b, w1, bf1, w2, bf2) = outs
        weights = ([wqkv, wproj], [w1, w2])
        vectors = ((n1g, n1b, bpj, bqv, n2g, n2b, bf2, bf1), ())
        for c in range(hidden_ref.shape[0]):
            lanes = slice(c * LANES, (c + 1) * LANES)
            out_ref[:, lanes] = hidden_ref[c].astype(BF)
            in_grad_ref[:, lanes] = grad_ref[c]
        for layer in range(LAYERS):
            for half in (ATTN, MLP):
                groups[half].emit(layer, blocks[2 * layer + half], weights[half], vectors[half])

    return pl.pallas_call(
        body,
        in_specs=[VM] * (2 + 2 * LAYERS),
        out_specs=[VM] * 14,
        out_shape=[SDS((dims.flat, dims.width), BF), SDS((dims.flat, dims.width), F32)] + [SDS(p.shape, F32) for p in params],
        compiler_params=params_of(),
        name="emit",
    )(hidden, grad, *[sums[layer, half] for layer in range(LAYERS) for half in (ATTN, MLP)])


def per_device(devices, inputs, out_grad, live_counts, *params):
    cube = Cube(devices)
    images, seq, width = inputs.shape
    dims = Dims(images, live_counts.shape[0], seq, width, params[9].shape[1] * devices)
    size = lambda *which: [params[i].shape[1] for i in which]
    groups = [
        Group(cube, [params[2].shape[1:], params[4].shape[1:]], size(0, 1, 5, 3, 6, 7, 11, 9)),
        Group(cube, [params[8].shape[1:], params[10].shape[1:]], []),
    ]
    lay = lambda a: a.transpose(1, 0, 2).reshape(dims.flat, width)
    unlay = lambda a: a.reshape(seq, images, width).transpose(1, 0, 2)
    turn = lambda a: a.transpose(1, 0, 2) if a.ndim == 3 and a.shape[1 if a.shape[0] == LAYERS else 0] % 8 else a
    turned = [turn(p) for p in params]
    hidden, whole, saved_attn, saved_mlp = forward(cube, dims, groups, live_counts, lay(inputs), turned)
    grad, sums = backward(cube, dims, groups, live_counts, lay(out_grad), whole, saved_attn, saved_mlp)
    outputs, in_grad, *grads = emit_outputs(dims, groups, hidden, grad, sums, turned)
    return (unlay(outputs), unlay(in_grad), *[turn(g) for g in grads])


def solution(mesh):
    devices = mesh.shape["fsdp"]
    rows3, flat2, rows2 = P("fsdp", None, None), P(None, "fsdp"), P(None, "fsdp", None)
    param_specs = (flat2, flat2, rows2, flat2, rows2, flat2, flat2, flat2, rows2, flat2, rows2, flat2)
    return jax.shard_map(
        functools.partial(per_device, devices),
        mesh=mesh,
        in_specs=(rows3, rows3, P("fsdp")) + param_specs,
        out_specs=(rows3, rows3) + param_specs,
        check_vma=False,
    )
```
